32 devices in a mesh: dp: 2 (over x), tp: 16 (over z, y, core).
Axes of the slice: x: 2, y: 2, z: 4, core: 2. Of those that a mesh axis runs over, the one named last changes fastest.
Arguments:
- token_ids: int32 [2, 256], P('dp'), parts along dimension 0
- embed_table: bfloat16 [8192, 4096], P('tp')
- emb_gain: float32 [4096], replicated
- emb_bias: float32 [4096], replicated
- ln1_gain: float32 [4096], replicated
- ln1_bias: float32 [4096], replicated
- w_qkv: bfloat16 [4096, 32, 3, 128], P(None, 'tp')
- b_qkv: float32 [32, 3, 128], P('tp')
- w_dense: bfloat16 [4096, 4096], P('tp')
- b_dense: float32 [4096], replicated
- ln2_gain: float32 [4096], replicated
- ln2_bias: float32 [4096], replicated
- w_fc1: bfloat16 [4096, 16384], P(None, 'tp')
- b_fc1: float32 [16384], P('tp')
- w_fc2: bfloat16 [16384, 4096], P('tp')
- b_fc2: float32 [4096], replicated
- d_out: bfloat16 [2, 256, 4096], P('dp', 'tp'), parts along dimension 0
Outputs:
- output 1: bfloat16 [2, 256, 4096], P('dp', 'tp'), parts along dimension 0
- output 2: float32 [16384, 4096], P(('dp', 'tp')), parts along dimension 0
- output 3: float32 [8192], P('dp'), parts along dimension 0
- output 4: float32 [8192], P('dp'), parts along dimension 0
- output 5: float32 [8192], P('dp'), parts along dimension 0
- output 6: float32 [8192], P('dp'), parts along dimension 0
- output 7: bfloat16 [8192, 32, 3, 128], P('dp', 'tp'), parts along dimension 0
- output 8: float32 [64, 3, 128], P(('dp', 'tp')), parts along dimension 0
- output 9: bfloat16 [8192, 4096], P(('dp', 'tp')), parts along dimension 0
- output 10: float32 [8192], P('dp'), parts along dimension 0
- output 11: float32 [8192], P('dp'), parts along dimension 0
- output 12: float32 [8192], P('dp'), parts along dimension 0
- output 13: bfloat16 [8192, 16384], P('dp', 'tp'), parts along dimension 0
- output 14: float32 [32768], P(('dp', 'tp')), parts along dimension 0
- output 15: bfloat16 [32768, 4096], P(('dp', 'tp')), parts along dimension 0
- output 16: float32 [8192], P('dp'), parts along dimension 0
There are 2 independent parts. The reference program is written for one: setup_inputs(seed, part) draws one part's arguments, and reference() takes and returns one part's arrays. A program takes and returns all parts, laid end to end along the dimension named above; an argument that names none is the same for every part.
All inputs are finite; a program needn't handle non-finite values.
Results may differ from the reference program's by a relative error of at most 0.02.
Values are sent between devices in bfloat16 or wider.
A program may use at most 1 GiB of HBM per device.

```python
import jax
import jax.numpy as jnp
from jax import lax

BATCH = 1
SEQ = 256
D_MODEL = 4096
HEADS = 32
VOCAB = 8192

HEAD_DIM = D_MODEL // HEADS
FFN = 4 * D_MODEL
EPS = 1e-5


def draw_ids(id_key):
    key_a, key_b, key_c, key_d = jax.random.split(id_key, 4)
    shape_ids = (BATCH, SEQ)
    upper_one = jax.random.randint(key_a, shape_ids, 1, VOCAB + 1)
    upper_two = jax.random.randint(key_b, shape_ids, 1, upper_one + 1)
    skewed = jax.random.randint(key_c, shape_ids, 0, upper_two)
    positions = jnp.arange(SEQ)
    stripe_lo = (positions // 4) * 4 * VOCAB // SEQ
    stripe_hi = (positions // 4 + 1) * 4 * VOCAB // SEQ
    spread = jax.random.randint(key_d, shape_ids, stripe_lo, stripe_hi)
    return jnp.where(positions % 4 == 0, spread, skewed).astype(jnp.int32)


def setup_inputs(seed: int = 0, part: int = 0) -> dict:
    root_key = jax.random.key(seed)
    part_key = jax.random.fold_in(root_key, part)
    key_list = jax.random.split(root_key, 15)
    id_key, grad_key = jax.random.split(part_key)

    def draw_normal(slot_num, shape_out, scale_by):
        return scale_by * jax.random.normal(key_list[slot_num], shape_out, jnp.float32)

    scale_in = D_MODEL ** -0.5
    scale_ff = FFN ** -0.5
    return {
        'token_ids': draw_ids(id_key),
        'embed_table': draw_normal(0, (VOCAB, D_MODEL), 1.0).astype(jnp.bfloat16),
        'emb_gain': 1.0 + draw_normal(1, (D_MODEL,), 0.25),
        'emb_bias': draw_normal(2, (D_MODEL,), 0.25),
        'ln1_gain': 1.0 + draw_normal(3, (D_MODEL,), 0.25),
        'ln1_bias': draw_normal(4, (D_MODEL,), 0.25),
        'w_qkv': draw_normal(5, (D_MODEL, HEADS, 3, HEAD_DIM), scale_in).astype(jnp.bfloat16),
        'b_qkv': draw_normal(6, (HEADS, 3, HEAD_DIM), 0.3),
        'w_dense': draw_normal(7, (D_MODEL, D_MODEL), scale_in).astype(jnp.bfloat16),
        'b_dense': draw_normal(8, (D_MODEL,), 0.3),
        'ln2_gain': 1.0 + draw_normal(9, (D_MODEL,), 0.25),
        'ln2_bias': draw_normal(10, (D_MODEL,), 0.25),
        'w_fc1': draw_normal(11, (D_MODEL, FFN), scale_in).astype(jnp.bfloat16),
        'b_fc1': draw_normal(12, (FFN,), 0.3),
        'w_fc2': draw_normal(13, (FFN, D_MODEL), scale_ff).astype(jnp.bfloat16),
        'b_fc2': draw_normal(14, (D_MODEL,), 0.3),
        'd_out': jax.random.normal(grad_key, (BATCH, SEQ, D_MODEL), jnp.float32).astype(jnp.bfloat16),
    }


def to_bf16(values):
    return values.astype(jnp.bfloat16).astype(jnp.float32)


def layer_norm(values, gain_vec, bias_vec):
    centered = values - jnp.mean(values, axis=-1, keepdims=True)
    var_val = jnp.mean(centered * centered, axis=-1, keepdims=True)
    return centered * lax.rsqrt(var_val + EPS) * gain_vec + bias_vec


def alibi_slopes():
    closest = 2 ** (HEADS.bit_length() - 1)
    slope_base = 2.0 ** (-8.0 / closest)
    extra_base = 2.0 ** (-4.0 / closest)
    slopes = [slope_base ** exponent for exponent in range(1, closest + 1)]
    slopes = slopes + [extra_base ** exponent for exponent in range(1, 2 * (HEADS - closest), 2)]
    return jnp.array(slopes, dtype=jnp.float32)


def seq_forward(x_seq, params):
    (emb_gain, emb_bias, ln1_gain, ln1_bias, w_qkv, b_qkv, w_dense, b_dense,
     ln2_gain, ln2_bias, w_fc1, b_fc1, w_fc2, b_fc2) = params
    embedded = to_bf16(layer_norm(x_seq, emb_gain, emb_bias))
    h_one = to_bf16(layer_norm(embedded, ln1_gain, ln1_bias))
    qkv_all = to_bf16(jnp.einsum('sd,dhce->shce', h_one, w_qkv) + b_qkv)
    positions = jnp.arange(SEQ)
    rel_pos = (positions[None, :] - positions[:, None]).astype(jnp.float32)
    causal = positions[None, :] <= positions[:, None]
    scores = jnp.einsum('qhe,khe->hqk', qkv_all[:, :, 0], qkv_all[:, :, 1]) * HEAD_DIM ** -0.5
    scores = jnp.where(causal, scores + alibi_slopes()[:, None, None] * rel_pos, -1e30)
    prob_bf = to_bf16(jax.nn.softmax(scores, axis=-1))
    context = to_bf16(jnp.einsum('hqk,khe->qhe', prob_bf, qkv_all[:, :, 2])).reshape(SEQ, D_MODEL)
    r_one = to_bf16(embedded + jnp.dot(context, w_dense, preferred_element_type=jnp.float32) + b_dense)
    h_two = to_bf16(layer_norm(r_one, ln2_gain, ln2_bias))
    gelu_out = to_bf16(jax.nn.gelu(jnp.dot(h_two, w_fc1, preferred_element_type=jnp.float32) + b_fc1, approximate=True))
    return to_bf16(r_one + jnp.dot(gelu_out, w_fc2, preferred_element_type=jnp.float32) + b_fc2)


def reference(token_ids, embed_table, emb_gain, emb_bias, ln1_gain, ln1_bias, w_qkv, b_qkv,
              w_dense, b_dense, ln2_gain, ln2_bias, w_fc1, b_fc1, w_fc2, b_fc2, d_out):
    params = tuple(weight.astype(jnp.float32) for weight in (
        emb_gain, emb_bias, ln1_gain, ln1_bias, w_qkv, b_qkv, w_dense, b_dense,
        ln2_gain, ln2_bias, w_fc1, b_fc1, w_fc2, b_fc2))
    x_zero = jnp.take(embed_table, token_ids, axis=0).astype(jnp.float32)

    def seq_step(grad_sum, step_in):
        x_seq, dy_seq = step_in
        y_seq, pull_back = jax.vjp(seq_forward, x_seq, params)
        dx_seq, d_params = pull_back(dy_seq.astype(jnp.float32))
        grad_sum = jax.tree.map(jnp.add, grad_sum, d_params)
        return grad_sum, (y_seq.astype(jnp.bfloat16), dx_seq.astype(jnp.bfloat16))

    grad_zero = jax.tree.map(jnp.zeros_like, params)
    grad_total, (y_out, dx_zero) = lax.scan(seq_step, grad_zero, (x_zero, d_out))
    d_table = jax.ops.segment_sum(dx_zero.astype(jnp.float32).reshape(BATCH * SEQ, D_MODEL),
                                  token_ids.reshape(BATCH * SEQ), num_segments=VOCAB)
    (d_emb_gain, d_emb_bias, d_ln1_gain, d_ln1_bias, d_w_qkv, d_b_qkv, d_w_dense, d_b_dense,
     d_ln2_gain, d_ln2_bias, d_w_fc1, d_b_fc1, d_w_fc2, d_b_fc2) = grad_total
    return (y_out, d_table, d_emb_gain, d_emb_bias, d_ln1_gain, d_ln1_bias,
            d_w_qkv.astype(jnp.bfloat16), d_b_qkv, d_w_dense.astype(jnp.bfloat16), d_b_dense,
            d_ln2_gain, d_ln2_bias, d_w_fc1.astype(jnp.bfloat16), d_b_fc1,
            d_w_fc2.astype(jnp.bfloat16), d_b_fc2)
```

```python
import functools
import jax
import jax.numpy as jnp
from jax import lax
from jax.experimental import pallas as pl
from jax.experimental.pallas import tpu as pltpu
from jax.sharding import PartitionSpec as P

EPS = 1e-5
MESH = pl.DeviceIdType.MESH
F32 = jnp.float32
BF16 = jnp.bfloat16
NCH = 4
NB = 16
BLK = 16
SEQ = 256
LANE = 128
QKV = 6 * LANE
ALL = slice(None)
GELU_A = 0.7978845608028654
GELU_B = 0.044715


def alibi_slopes(head_count):
    closest = 2 ** (head_count.bit_length() - 1)
    slope_base = 2.0 ** (-8.0 / closest)
    extra_base = 2.0 ** (-4.0 / closest)
    slopes = [slope_base ** exponent for exponent in range(1, closest + 1)]
    slopes = slopes + [extra_base ** exponent for exponent in range(1, 2 * (head_count - closest), 2)]
    return jnp.array(slopes, dtype=jnp.float32)


def norm_forward(values, gain_vec, bias_vec):
    centered = values - jnp.mean(values, axis=-1, keepdims=True)
    inv_std = lax.rsqrt(jnp.mean(centered * centered, axis=-1, keepdims=True) + EPS)
    x_hat = centered * inv_std
    return x_hat * gain_vec + bias_vec, x_hat, inv_std


def norm_backward(d_norm, x_hat, inv_std, gain_vec):
    d_hat = d_norm * gain_vec
    d_values = inv_std * (d_hat - jnp.mean(d_hat, axis=-1, keepdims=True)
                          - x_hat * jnp.mean(d_hat * x_hat, axis=-1, keepdims=True))
    return d_values, jnp.sum(d_norm * x_hat, axis=0, keepdims=True), jnp.sum(d_norm, axis=0, keepdims=True)


def dot_nn(a, b):
    return lax.dot_general(a, b, (((1,), (0,)), ((), ())), preferred_element_type=F32)


def dot_nt(a, b):
    return lax.dot_general(a, b, (((1,), (1,)), ((), ())), preferred_element_type=F32)


def dot_tn(a, b):
    return lax.dot_general(a, b, (((0,), (0,)), ((), ())), preferred_element_type=F32)


class Place:
    def __init__(self):
        t = lax.axis_index('tp')
        self.t = t
        self.c = lax.rem(t, 2)
        self.y = lax.rem(lax.div(t, 2), 2)
        self.z = lax.div(t, 4)
        self.sib = t + 1 - 2 * self.c
        self.yp = t + 2 - 4 * self.y
        self.zs = [self.z, self.z + 1 - 2 * lax.rem(self.z, 2), lax.rem(self.z + 2, 4), 3 - self.z]
        self.tz = [zk * 4 + self.y * 2 + self.c for zk in self.zs]
        self.own = self.c * 8 + self.y * 4
        self.oth = self.c * 8 + (1 - self.y) * 4
        self.me = self.own + self.z


class Gather:
    def __init__(self, pc, buf, send, recv, nch):
        self.pc, self.buf, self.send, self.recv, self.nch = pc, buf, send, recv, nch
        self.cw = buf.shape[2] // nch

    def rc(self, first, count, ch, slot, dev):
        ref = self.buf.at[pl.ds(first, count), :, pl.ds(pl.multiple_of(ch * self.cw, self.cw), self.cw)]
        return pltpu.make_async_remote_copy(
            src_ref=ref, dst_ref=ref, send_sem=self.send.at[ch, slot], recv_sem=self.recv.at[ch, slot],
            device_id={'tp': dev}, device_id_type=MESH)

    def start(self):
        pc = self.pc

        def body(ch, _):
            self.rc(pc.me, 1, ch, 3, pc.yp).start()
            for k in (1, 2, 3):
                self.rc(pc.me, 1, ch, k - 1, pc.tz[k]).start()
            return 0
        lax.fori_loop(0, self.nch, body, 0)

    def a(self, ch):
        pc = self.pc
        for k in (1, 2, 3):
            self.rc(pc.own + pc.zs[k], 1, ch, k - 1, pc.tz[k]).wait_recv()
            self.rc(pc.own + pc.zs[k], 1, ch, 3 + k, pc.yp).start()
        self.rc(pc.own, 4, ch, 7, pc.sib).start()

    def b(self, ch):
        pc = self.pc
        for k in (0, 1, 2, 3):
            self.rc(pc.oth + pc.zs[k], 1, ch, 3 + k, pc.yp).wait_recv()
        self.rc(pc.oth, 4, ch, 8, pc.sib).start()

    def c(self, ch):
        pc = self.pc
        self.rc(pc.own, 4, ch, 7, pc.sib).wait_recv()
        self.rc(pc.oth, 4, ch, 8, pc.sib).wait_recv()

    def finish(self):
        pc = self.pc

        def body(ch, _):
            for slot in range(7):
                self.rc(pc.me, 1, ch, slot, pc.yp).wait_send()
            for slot in (7, 8):
                self.rc(pc.own, 4, ch, slot, pc.sib).wait_send()
            return 0
        lax.fori_loop(0, self.nch, body, 0)

    def run(self, consume, hook=None):
        def body(s, _):
            @pl.when(s < self.nch)
            def _():
                self.a(s)

            @pl.when((s >= 1) & (s <= self.nch))
            def _():
                self.b(s - 1)

            if hook is not None:
                hook(s)

            @pl.when(s >= 2)
            def _():
                self.c(s - 2)
                if consume is not None:
                    consume(s - 2)
            return 0
        lax.fori_loop(0, self.nch + 2, body, 0)
        self.finish()


class Scatter:
    def __init__(self, pc, part, bufs, send, recv, out):
        self.pc, self.part, self.send, self.recv, self.out = pc, part, send, recv, out
        self.ra, self.sb, self.rb, self.sc, self.rcv = bufs
        self.cw = part.shape[2] // NCH

    def cols(self, ch):
        return pl.ds(pl.multiple_of(ch * self.cw, self.cw), self.cw)

    def copy(self, src, dst, ch, slot, dev):
        return pltpu.make_async_remote_copy(
            src_ref=src, dst_ref=dst, send_sem=self.send.at[ch, slot], recv_sem=self.recv.at[ch, slot],
            device_id={'tp': dev}, device_id_type=MESH)

    def to_sib(self, ch):
        pc = self.pc
        return self.copy(self.part.at[pl.ds((1 - pc.c) * 8, 8), :, self.cols(ch)],
                         self.ra.at[:, :, self.cols(ch)], ch, 0, pc.sib)

    def to_y(self, ch):
        return self.copy(self.sb.at[:, :, self.cols(ch)], self.rb.at[:, :, self.cols(ch)], ch, 1, self.pc.yp)

    def to_z(self, ch, k):
        return self.copy(self.sc.at[k - 1, :, self.cols(ch)], self.rcv.at[k - 1, :, self.cols(ch)],
                         ch, 1 + k, self.pc.tz[k])

    def s0(self, ch):
        self.to_sib(ch).start()

    def s1(self, ch):
        pc, cols = self.pc, self.cols(ch)
        self.to_sib(ch).wait_recv()
        for k in range(4):
            self.sb[k, :, cols] = (self.part[pc.oth + k, :, cols].astype(F32)
                                   + self.ra[(1 - pc.y) * 4 + k, :, cols].astype(F32)).astype(BF16)
        self.to_y(ch).start()

    def pair(self, zk, cols):
        pc = self.pc
        return (self.part[pc.own + zk, :, cols].astype(F32) + self.ra[pc.y * 4 + zk, :, cols].astype(F32)
                + self.rb[zk, :, cols].astype(F32))

    def s2(self, ch):
        pc, cols = self.pc, self.cols(ch)
        self.to_y(ch).wait_recv()
        for k in (2, 3, 1):
            self.sc[k - 1, :, cols] = self.pair(pc.zs[k], cols).astype(BF16)
            self.to_z(ch, k).start()

    def s3(self, ch):
        pc, cols = self.pc, self.cols(ch)
        acc = self.pair(pc.z, cols)
        for k in (1, 2, 3):
            self.to_z(ch, k).wait_recv()
            acc = acc + self.rcv[k - 1, :, cols].astype(F32)
        self.out[:, cols] = acc

    def finish(self):
        def body(ch, _):
            self.to_sib(ch).wait_send()
            self.to_y(ch).wait_send()
            for k in (1, 2, 3):
                self.to_z(ch, k).wait_send()
            return 0
        lax.fori_loop(0, NCH, body, 0)

    def run(self, compute, hook=None):
        def body(s, _):
            @pl.when(s < NCH)
            def _():
                compute(s)
                self.s0(s)

            @pl.when((s >= 1) & (s <= NCH))
            def _():
                self.s1(s - 1)

            if hook is not None:
                hook(s)

            @pl.when((s >= 2) & (s <= NCH + 1))
            def _():
                self.s2(s - 2)

            @pl.when(s >= 3)
            def _():
                self.s3(s - 3)
            return 0
        lax.fori_loop(0, NCH + 3, body, 0)
        self.finish()


def chain_kernel(ids, slopes, eg, eb, g1, b1, g2, b2, bd, bf2, bqkv, bf1, dout,
                 table_h, wqkv_h, wd_h, w1_h, w2_h,
                 h1_o, h2_o, dy_o, dr_o, dx_o, ctx_o, gelu_o, dpre_o, dqkv_o, y_o, small_o, dbf1_o, dbqkv_o,
                 table, wraw, wq, wd, w1, w2, h1, h2, dy, dr, dx, st2, st4, part, party,
                 ra, sb, rb, sc, rcv, yra, ysb, yrb, ysc, yrcv,
                 onehot, wstage, qkv_acc, qkv, prob, ctx, pre, dgelu, gelu_bf, dpre, dqkv,
                 rsum, e_val, e_hat, n1_hat, n2_hat, r_one, dr_own, invs,
                 lsem, osem, ags, agr, agds, agdr, rss, rsr, rsys, rsyr, sts, strc):
    pc = Place()
    dim = table.shape[1]
    vocab_rows = table.shape[0]
    cw = dim // NCH

    loads = [pltpu.make_async_copy(table_h, table, lsem.at[0]),
             pltpu.make_async_copy(wd_h, wd, lsem.at[1]),
             pltpu.make_async_copy(w1_h, w1, lsem.at[2]),
             pltpu.make_async_copy(w2_h, w2, lsem.at[3])]
    raw_rows = wraw.shape[1]

    def raw_load(ch, slot):
        return pltpu.make_async_copy(wqkv_h.at[pl.ds(pl.multiple_of(ch * raw_rows, raw_rows), raw_rows), :],
                                     wraw.at[slot], lsem.at[4 + slot])

    loads[0].start()
    raw_load(0, 0).start()
    raw_load(1, 1).start()
    for cp in loads[1:]:
        cp.start()

    barrier = pltpu.get_barrier_semaphore()
    partners = [pc.sib, pc.yp] + pc.tz[1:]
    for dev in partners:
        pl.semaphore_signal(barrier, inc=1, device_id={'tp': dev}, device_id_type=MESH)

    local_ids = ids[ALL] - pc.t * vocab_rows
    onehot[ALL] = (local_ids == lax.broadcasted_iota(jnp.int32, (SEQ, vocab_rows), 1)).astype(F32).astype(BF16)
    pl.semaphore_wait(barrier, len(partners))
    loads[0].wait()

    def cols(ch):
        return pl.ds(pl.multiple_of(ch * cw, cw), cw)

    def blocks(value):
        return value.reshape(NB, BLK, value.shape[1])

    def rows(value):
        return value.reshape(SEQ, value.shape[2])

    main = (ra, sb, rb, sc, rcv)
    side = (yra, ysb, yrb, ysc, yrcv)
    scatter = Scatter(pc, part, main, rss, rsr, rsum)
    scatter_y = Scatter(pc, party, side, rsys, rsyr, rsum)

    def embed(ch):
        part[:, :, cols(ch)] = blocks(dot_nn(onehot[ALL], table[:, cols(ch)]).astype(BF16))

    def unpack_wqkv(s):
        @pl.when(s < NCH)
        def _():
            slot = lax.rem(s, 2)
            raw_load(s, slot).wait()

            def body(i, _):
                wstage[ALL] = wraw[slot, pl.ds(pl.multiple_of(i * QKV, QKV), QKV), :].astype(F32)
                out_row = pl.multiple_of(s * cw + i * LANE, LANE)
                for j in range(6):
                    wq[pl.ds(out_row, LANE), j * LANE:(j + 1) * LANE] = wstage[pl.ds(j, LANE, stride=6), :].astype(BF16)
                return 0
            lax.fori_loop(0, raw_rows // QKV, body, 0)

            @pl.when(s + 2 < NCH)
            def _():
                raw_load(s + 2, slot).start()

    scatter.run(embed, unpack_wqkv)
    e_norm, hat, inv = norm_forward(rsum[ALL], eg[ALL], eb[ALL])
    e_hat[ALL] = hat
    invs[0] = jnp.broadcast_to(inv, (BLK, LANE))
    embedded = e_norm.astype(BF16).astype(F32)
    e_val[ALL] = embedded
    n1_norm, hat, inv = norm_forward(embedded, g1[ALL], b1[ALL])
    n1_hat[ALL] = hat
    invs[1] = jnp.broadcast_to(inv, (BLK, LANE))
    h1[pc.me] = n1_norm.astype(BF16)

    gather = Gather(pc, h1, ags, agr, NCH)
    gather.start()
    dy[pc.me] = dout[ALL]
    qkv_acc[ALL] = jnp.zeros_like(qkv_acc)

    def use_h1(ch):
        qkv_acc[ALL] += dot_nn(rows(h1[:, :, cols(ch)]), wq[cols(ch), :])

    gather.run(use_h1)
    gather_dy = Gather(pc, dy, agds, agdr, NCH)
    gather_dy.start()
    out_h1 = pltpu.make_async_copy(h1, h1_o, osem.at[0])
    out_h1.start()

    def position(axis):
        r = lax.broadcasted_iota(jnp.int32, (SEQ, SEQ), axis)
        core, yy = lax.shift_right_logical(r, 7), lax.shift_right_logical(r, 6) & 1
        zz, w = lax.shift_right_logical(r, 4) & 3, r & 15
        return zz * 64 + yy * 32 + core * 16 + w

    q_pos, k_pos = position(0), position(1)
    rel = (k_pos - q_pos).astype(F32)
    causal = k_pos <= q_pos
    scale = LANE ** -0.5

    for j in range(6):
        qkv[:, j * LANE:(j + 1) * LANE] = (qkv_acc[:, j * LANE:(j + 1) * LANE] + bqkv[j // 2, j % 2:j % 2 + 1, :]).astype(BF16)

    def head_cols(kind, h):
        return slice((kind * 2 + h) * LANE, (kind * 2 + h + 1) * LANE)

    def attend(h):
        scores = dot_nt(qkv[:, head_cols(0, h)], qkv[:, head_cols(1, h)]) * scale
        scores = jnp.where(causal, scores + slopes[pc.t * 2 + h] * rel, -1e30)
        ex = jnp.exp(scores - jnp.max(scores, axis=-1, keepdims=True))
        p = ex / jnp.sum(ex, axis=-1, keepdims=True)
        prob[h] = p
        ctx[:, h * LANE:(h + 1) * LANE] = dot_nn(p.astype(BF16), qkv[:, head_cols(2, h)]).astype(BF16)

    attend(0)
    lax.fori_loop(0, NCH, lambda ch, u: (gather_dy.a(ch), u)[1], 0)
    attend(1)
    loads[1].wait()

    def dense(ch):
        part[:, :, cols(ch)] = blocks(dot_nn(ctx[ALL], wd[:, cols(ch)]).astype(BF16))

    dgelu[ALL] = jnp.zeros_like(dgelu)
    loads[3].wait()

    def use_dy(s):
        @pl.when(s < NCH)
        def _():
            gather_dy.b(s)

        @pl.when((s >= 1) & (s <= NCH))
        def _():
            gather_dy.c(s - 1)
            dgelu[ALL] += dot_nt(rows(dy[:, :, cols(s - 1)]), w2[:, cols(s - 1)])

    scatter.run(dense, use_dy)
    gather_dy.finish()
    out_dy = pltpu.make_async_copy(dy, dy_o, osem.at[1])
    out_dy.start()
    out_ctx = pltpu.make_async_copy(ctx, ctx_o, osem.at[2])
    out_ctx.start()

    r_val = (e_val[ALL] + rsum[ALL] + bd[ALL]).astype(BF16).astype(F32)
    r_one[ALL] = r_val
    n2_norm, hat, inv = norm_forward(r_val, g2[ALL], b2[ALL])
    n2_hat[ALL] = hat
    invs[2] = jnp.broadcast_to(inv, (BLK, LANE))
    h2[pc.me] = n2_norm.astype(BF16)
    gather = Gather(pc, h2, ags, agr, NCH)
    gather.start()
    pre[ALL] = jnp.zeros_like(pre)
    loads[2].wait()

    def use_h2(ch):
        pre[ALL] += dot_nn(rows(h2[:, :, cols(ch)]), w1[cols(ch), :])

    gather.run(use_h2)
    out_h2 = pltpu.make_async_copy(h2, h2_o, osem.at[3])
    out_h2.start()

    def act(i, total):
        rs = pl.ds(pl.multiple_of(i * 32, 32), 32)
        x = pre[rs, :] + bf1[ALL]
        th = jnp.tanh(GELU_A * (x + GELU_B * (x * x * x)))
        cdf = 0.5 * (1.0 + th)
        gelu_bf[rs, :] = (x * cdf).astype(BF16)
        slope = cdf + x * (0.5 * (1.0 - th * th)) * (GELU_A * (1.0 + 3.0 * GELU_B * (x * x)))
        d = dgelu[rs, :] * slope
        dpre[rs, :] = d.astype(BF16)
        return total + jnp.sum(d, axis=0, keepdims=True)

    dbf1_o[ALL] = lax.fori_loop(0, SEQ // 32, act, jnp.zeros((1, pre.shape[1]), F32))
    out_gelu = pltpu.make_async_copy(gelu_bf, gelu_o, osem.at[4])
    out_gelu.start()
    out_dpre = pltpu.make_async_copy(dpre, dpre_o, osem.at[5])
    out_dpre.start()

    def dh2(ch):
        part[:, :, cols(ch)] = blocks(dot_nt(dpre[ALL], w1[cols(ch), :]).astype(BF16))

    def mlp(s):
        @pl.when(s < NCH)
        def _():
            party[:, :, cols(s)] = blocks(dot_nn(gelu_bf[ALL], w2[:, cols(s)]).astype(BF16))

    scatter.run(dh2, mlp)
    dn, sg, sbv = norm_backward(rsum[ALL], n2_hat[ALL], invs[2, :, 0:1], g2[ALL])
    dr_val = dout[ALL].astype(F32) + dn
    dr_own[ALL] = dr_val
    dr[pc.me] = dr_val.astype(BF16)
    st2[pc.me] = jnp.concatenate([sg, sbv], axis=0).astype(BF16)
    gather = Gather(pc, dr, ags, agr, NCH)
    gather.start()
    gather_st = Gather(pc, st2, sts, strc, 1)
    gather_st.start()
    d_ctx = qkv_acc.at[:, 0:256]
    d_ctx[ALL] = jnp.zeros((SEQ, 256), F32)

    def use_dr(ch):
        d_ctx[ALL] += dot_nt(rows(dr[:, :, cols(ch)]), wd[:, cols(ch)])

    def y_start(s):
        @pl.when(s < NCH)
        def _():
            scatter_y.s0(s)

    gather.run(use_dr, y_start)
    out_dr = pltpu.make_async_copy(dr, dr_o, osem.at[6])
    out_dr.start()
    gather_st.a(0)
    lax.fori_loop(0, NCH, lambda ch, u: (scatter_y.s1(ch), u)[1], 0)
    gather_st.b(0)

    def attend_back(h):
        dc = d_ctx[:, h * LANE:(h + 1) * LANE].astype(BF16)
        p = prob[h]
        d_value = dot_tn(p.astype(BF16), dc)
        d_prob = dot_nt(dc, qkv[:, head_cols(2, h)])
        ds = p * (d_prob - jnp.sum(d_prob * p, axis=-1, keepdims=True))
        ds_bf = (ds * scale).astype(BF16)
        d_query = dot_nn(ds_bf, qkv[:, head_cols(1, h)])
        d_key = dot_tn(ds_bf, qkv[:, head_cols(0, h)])
        for kind, val in ((0, d_query), (1, d_key), (2, d_value)):
            dqkv[:, head_cols(kind, h)] = val.astype(BF16)
            dbqkv_o[kind, h:h + 1, :] = jnp.sum(val, axis=0, keepdims=True)

    attend_back(0)
    attend_back(1)
    out_dqkv = pltpu.make_async_copy(dqkv, dqkv_o, osem.at[7])
    out_dqkv.start()
    lax.fori_loop(0, NCH, lambda ch, u: (scatter_y.s2(ch), u)[1], 0)

    gather_st.c(0)
    gather_st.finish()

    def dh1(ch):
        part[:, :, cols(ch)] = blocks(dot_nt(dqkv[ALL], wq[cols(ch), :]).astype(BF16))

    scatter.run(dh1)
    dn, sg1, sb1 = norm_backward(rsum[ALL], n1_hat[ALL], invs[1, :, 0:1], g1[ALL])
    dxv, sg0, sb0 = norm_backward(dr_own[ALL] + dn, e_hat[ALL], invs[0, :, 0:1], eg[ALL])
    dx[pc.me] = dxv.astype(BF16)
    st4[pc.me] = jnp.concatenate([sg0, sb0, sg1, sb1], axis=0).astype(BF16)
    gather = Gather(pc, dx, ags, agr, NCH)
    gather.start()
    gather_st = Gather(pc, st4, sts, strc, 1)
    gather_st.start()

    lax.fori_loop(0, NCH, lambda ch, u: (scatter_y.s3(ch), u)[1], 0)
    scatter_y.finish()
    y_o[ALL] = (r_one[ALL] + rsum[ALL] + bf2[ALL]).astype(BF16)
    small_o[4:6, :] = jnp.sum(st2[ALL].astype(F32), axis=0)

    def col_sums(s):
        @pl.when(s < NCH)
        def _():
            small_o[6:7, cols(s)] = jnp.sum(rows(dr[:, :, cols(s)]).astype(F32), axis=0, keepdims=True)
            small_o[7:8, cols(s)] = jnp.sum(rows(dy[:, :, cols(s)]).astype(F32), axis=0, keepdims=True)

    gather.run(None, col_sums)
    gather_st.a(0)
    gather_st.b(0)
    gather_st.c(0)
    gather_st.finish()
    small_o[0:4, :] = jnp.sum(st4[ALL].astype(F32), axis=0)
    out_dx = pltpu.make_async_copy(dx, dx_o, osem.at[8])
    out_dx.start()
    for cp in (out_h1, out_dy, out_ctx, out_h2, out_gelu, out_dpre, out_dr, out_dqkv, out_dx):
        cp.wait()


def chain(ids, slopes, vecs, bqkv, bf1, dout, table, wqkv, wd, w1, w2):
    vocab_rows, dim = table.shape
    ff = w1.shape[1]
    act = jax.ShapeDtypeStruct((NB, BLK, dim), BF16)
    out_shape = [act] * 5 + [
        jax.ShapeDtypeStruct((SEQ, 256), BF16), jax.ShapeDtypeStruct((SEQ, ff), BF16),
        jax.ShapeDtypeStruct((SEQ, ff), BF16), jax.ShapeDtypeStruct((SEQ, QKV), BF16),
        jax.ShapeDtypeStruct((BLK, dim), BF16), jax.ShapeDtypeStruct((8, dim), F32),
        jax.ShapeDtypeStruct((1, ff), F32), jax.ShapeDtypeStruct((3, 2, LANE), F32)]
    vmem, hbm = pl.BlockSpec(memory_space=pltpu.VMEM), pl.BlockSpec(memory_space=pl.ANY)
    full = pltpu.VMEM((NB, BLK, dim), BF16)
    rs_bufs = [pltpu.VMEM((8, BLK, dim), BF16), pltpu.VMEM((4, BLK, dim), BF16), pltpu.VMEM((4, BLK, dim), BF16),
               pltpu.VMEM((3, BLK, dim), BF16), pltpu.VMEM((3, BLK, dim), BF16)]
    row = pltpu.VMEM((BLK, dim), F32)
    dma = pltpu.SemaphoreType.DMA
    scratch = [pltpu.VMEM((vocab_rows, dim), BF16), pltpu.VMEM((2, dim * 6 // NCH, LANE), BF16),
               pltpu.VMEM((dim, QKV), BF16), pltpu.VMEM(wd.shape, BF16), pltpu.VMEM(w1.shape, BF16),
               pltpu.VMEM(w2.shape, BF16), full, full, full, full, full,
               pltpu.VMEM((NB, 2, dim), BF16), pltpu.VMEM((NB, 4, dim), BF16), full, full]
    scratch += rs_bufs + rs_bufs
    scratch += [pltpu.VMEM((SEQ, vocab_rows), BF16), pltpu.VMEM((QKV, LANE), F32), pltpu.VMEM((SEQ, QKV), F32),
                pltpu.VMEM((SEQ, QKV), BF16), pltpu.VMEM((2, SEQ, SEQ), F32), pltpu.VMEM((SEQ, 256), BF16),
                pltpu.VMEM((SEQ, ff), F32), pltpu.VMEM((SEQ, ff), F32), pltpu.VMEM((SEQ, ff), BF16),
                pltpu.VMEM((SEQ, ff), BF16), pltpu.VMEM((SEQ, QKV), BF16)]
    scratch += [row] * 7 + [pltpu.VMEM((3, BLK, LANE), F32)]
    scratch += [dma((6,)), dma((9,)), dma((NCH, 9)), dma((NCH, 9)), dma((NCH, 9)), dma((NCH, 9)),
                dma((NCH, 5)), dma((NCH, 5)), dma((NCH, 5)), dma((NCH, 5)), dma((1, 9)), dma((1, 9))]
    return pl.pallas_call(
        chain_kernel, out_shape=out_shape,
        in_specs=[vmem, pl.BlockSpec(memory_space=pltpu.SMEM)] + [vmem] * 11 + [hbm] * 5,
        out_specs=[hbm] * 9 + [vmem] * 4,
        scratch_shapes=scratch, name='chain',
        compiler_params=pltpu.CompilerParams(collective_id=1, has_side_effects=True,
                                             vmem_limit_bytes=67043328),
    )(ids, slopes, *vecs, bqkv, bf1, dout, table, wqkv, wd, w1, w2)


def qkv_grad_kernel(h1, dqkv, out, stage):
    n = h1.shape[1]
    for j in range(6):
        stage[pl.ds(j, n, stride=6), :] = dot_tn(h1[ALL], dqkv[:, j * LANE:(j + 1) * LANE])
    out[ALL] = stage[ALL].astype(BF16)


def qkv_grad(h1, dqkv):
    dim = h1.shape[1]
    step = 512
    return pl.pallas_call(
        qkv_grad_kernel, out_shape=jax.ShapeDtypeStruct((dim * 6, LANE), BF16), grid=(dim // step,),
        in_specs=[pl.BlockSpec((SEQ, step), lambda i: (0, i)), pl.BlockSpec((SEQ, QKV), lambda i: (0, 0))],
        out_specs=pl.BlockSpec((step * 6, LANE), lambda i: (i, 0)),
        scratch_shapes=[pltpu.VMEM((step * 6, LANE), F32)], name='qkv_grad')(h1, dqkv)


def device_step(token_ids, embed_table, emb_gain, emb_bias, ln1_gain, ln1_bias,
                w_qkv, b_qkv, w_dense, b_dense, ln2_gain, ln2_bias,
                w_fc1, b_fc1, w_fc2, b_fc2, d_out, slopes_all):
    dim = embed_table.shape[1]
    vocab_rows = embed_table.shape[0]
    ids = token_ids.reshape(4, 2, 2, BLK).transpose(2, 1, 0, 3).reshape(SEQ, 1)
    vecs = [v.reshape(1, dim) for v in (emb_gain, emb_bias, ln1_gain, ln1_bias, ln2_gain, ln2_bias, b_dense, b_fc2)]
    wqkv = w_qkv.transpose(0, 2, 1, 3).reshape(dim * 6, LANE)
    (h1, h2, dy, dr, dx, ctx, gelu, dpre, dqkv, y, small, dbf1, dbqkv) = chain(
        ids, slopes_all, vecs, b_qkv.transpose(1, 0, 2), b_fc1.reshape(1, -1), d_out.reshape(BLK, dim),
        embed_table, wqkv, w_dense, w_fc1, w_fc2)
    h1, h2, dy, dr, dx = (v.reshape(SEQ, dim) for v in (h1, h2, dy, dr, dx))
    d_w_qkv = qkv_grad(h1, dqkv).reshape(dim, 3, 2, LANE).transpose(0, 2, 1, 3)
    d_w_fc2 = dot_tn(gelu, dy).astype(BF16)
    d_w_fc1 = dot_tn(h2, dpre).astype(BF16)
    d_w_dense = dot_tn(ctx, dr).astype(BF16)
    one_hot = (ids - lax.axis_index('tp') * vocab_rows == jnp.arange(vocab_rows)[None, :]).astype(BF16)
    d_table = dot_tn(one_hot, dx)
    return (y[None], d_table, small[0], small[1], small[2], small[3],
            d_w_qkv, dbqkv.transpose(1, 0, 2), d_w_dense, small[6], small[4], small[5],
            d_w_fc1, dbf1.reshape(-1), d_w_fc2, small[7])


def solution(mesh):
    in_specs = (P('dp', None), P('tp', None), P(None), P(None), P(None), P(None),
                P(None, 'tp', None, None), P('tp', None, None), P('tp', None), P(None),
                P(None), P(None), P(None, 'tp'), P('tp'), P('tp', None), P(None),
                P('dp', 'tp', None), P(None))
    out_specs = (P('dp', 'tp', None), P(('dp', 'tp'), None), P('dp'), P('dp'), P('dp'), P('dp'),
                 P('dp', 'tp', None, None), P(('dp', 'tp'), None, None), P(('dp', 'tp'), None), P('dp'),
                 P('dp'), P('dp'), P('dp', 'tp'), P(('dp', 'tp')), P(('dp', 'tp'), None), P('dp'))
    mapped = jax.shard_map(device_step, mesh=mesh, in_specs=in_specs, out_specs=out_specs, check_vma=False)

    def run(*arrays):
        slopes_all = alibi_slopes(arrays[6].shape[1])
        return mapped(*arrays, slopes_all)

    return run
```

```python
import functools
import jax
import jax.numpy as jnp
from jax import lax
from jax.experimental import pallas as pl
from jax.experimental.pallas import tpu as pltpu
from jax.sharding import PartitionSpec as P

EPS = 1e-5
MESH = pl.DeviceIdType.MESH
F32 = jnp.float32
BF16 = jnp.bfloat16
NA = 4
NR = 4
NW = 4
NB = 16
BLK = 16
SEQ = 256
LANE = 128
QKV = 6 * LANE
ALL = slice(None)
GELU_A = 0.7978845608028654
GELU_B = 0.044715


def alibi_slopes(head_count):
    closest = 2 ** (head_count.bit_length() - 1)
    slope_base = 2.0 ** (-8.0 / closest)
    extra_base = 2.0 ** (-4.0 / closest)
    slopes = [slope_base ** exponent for exponent in range(1, closest + 1)]
    slopes = slopes + [extra_base ** exponent for exponent in range(1, 2 * (head_count - closest), 2)]
    return jnp.array(slopes, dtype=jnp.float32)


def norm_forward(values, gain_vec, bias_vec):
    centered = values - jnp.mean(values, axis=-1, keepdims=True)
    inv_std = lax.rsqrt(jnp.mean(centered * centered, axis=-1, keepdims=True) + EPS)
    x_hat = centered * inv_std
    return x_hat * gain_vec + bias_vec, x_hat, inv_std


def norm_backward(d_norm, x_hat, inv_std, gain_vec):
    d_hat = d_norm * gain_vec
    d_values = inv_std * (d_hat - jnp.mean(d_hat, axis=-1, keepdims=True)
                          - x_hat * jnp.mean(d_hat * x_hat, axis=-1, keepdims=True))
    return d_values, jnp.sum(d_norm * x_hat, axis=0, keepdims=True), jnp.sum(d_norm, axis=0, keepdims=True)


def dot_nn(a, b):
    return lax.dot_general(a, b, (((1,), (0,)), ((), ())), preferred_element_type=F32)


def dot_nt(a, b):
    return lax.dot_general(a, b, (((1,), (1,)), ((), ())), preferred_element_type=F32)


def dot_tn(a, b):
    return lax.dot_general(a, b, (((0,), (0,)), ((), ())), preferred_element_type=F32)


class Place:
    def __init__(self):
        t = lax.axis_index('tp')
        self.t = t
        self.c = lax.rem(t, 2)
        self.y = lax.rem(lax.div(t, 2), 2)
        self.z = lax.div(t, 4)
        self.inner = (self.z == 1) | (self.z == 2)
        self.end = (self.z == 0) | (self.z == 3)
        self.sib = t + 1 - 2 * self.c
        self.yp = t + 2 - 4 * self.y
        self.zs = [self.z, self.z + 1 - 2 * lax.rem(self.z, 2), lax.rem(self.z + 2, 4), 3 - self.z]
        self.tz = [zk * 4 + self.y * 2 + self.c for zk in self.zs]
        self.own = self.c * 8 + self.y * 4
        self.oth = self.c * 8 + (1 - self.y) * 4
        self.me = self.own + self.z


def remote(src, dst, send_sem, recv_sem, dev):
    return pltpu.make_async_remote_copy(src_ref=src, dst_ref=dst, send_sem=send_sem, recv_sem=recv_sem,
                                        device_id={'tp': dev}, device_id_type=MESH)


def loop(n, fn):
    def body(i, carry):
        fn(i)
        return carry
    lax.fori_loop(0, n, body, 0)


class Gather:
    def __init__(self, pc, buf, send, recv):
        self.pc, self.buf, self.send, self.recv = pc, buf, send, recv
        self.cw = buf.shape[2] // NA

    def rc(self, first, count, ch, slot, dev, send_slot=None):
        ref = self.buf.at[pl.ds(first, count), :, pl.ds(pl.multiple_of(ch * self.cw, self.cw), self.cw)]
        send_slot = slot if send_slot is None else send_slot
        return remote(ref, ref, self.send.at[ch, send_slot], self.recv.at[ch, slot], dev)

    def block(self, k, ch):
        return self.rc(self.pc.own + self.pc.zs[k], 1, ch, k - 1, self.pc.tz[k])

    def start_y(self):
        loop(NA, lambda ch: self.rc(self.pc.me, 1, ch, 3, self.pc.yp).start())

    def start_z(self):
        pc = self.pc

        def body(ch):
            self.rc(pc.me, 1, ch, 0, pc.tz[1]).start()

            @pl.when(pc.inner)
            def _():
                self.rc(pc.me, 1, ch, 2, pc.tz[3]).start()

            @pl.when(pc.end)
            def _():
                self.rc(pc.me, 1, ch, 1, pc.tz[2]).start()
        loop(NA, body)

    def start(self):
        self.start_y()
        self.start_z()

    def to_y(self, k, ch):
        self.rc(self.pc.own + self.pc.zs[k], 1, ch, 3 + k, self.pc.yp).start()

    def to_end(self, k, ch):
        self.rc(self.pc.own + self.pc.zs[k], 1, ch, 4 - k, self.pc.tz[1], 7 + k).start()

    def a(self, ch):
        pc = self.pc
        self.block(1, ch).wait_recv()
        self.to_y(1, ch)

        @pl.when(pc.inner)
        def _():
            for k in (3, 2):
                self.block(k, ch).wait_recv()
                self.to_end(k, ch)
                self.to_y(k, ch)

        @pl.when(pc.end)
        def _():
            for k in (2, 3):
                self.block(k, ch).wait_recv()
                self.to_y(k, ch)
        self.rc(pc.own, 4, ch, 7, pc.sib).start()

    def b(self, ch):
        pc = self.pc
        for k in range(4):
            self.rc(pc.oth + pc.zs[k], 1, ch, 3 + k, pc.yp).wait_recv()
        self.rc(pc.oth, 4, ch, 8, pc.sib).start()

    def c(self, ch):
        pc = self.pc
        self.rc(pc.own, 4, ch, 7, pc.sib).wait_recv()
        self.rc(pc.oth, 4, ch, 8, pc.sib).wait_recv()

    def finish(self):
        pc = self.pc

        def body(ch):
            for slot in (0, 3, 4, 5, 6):
                self.rc(pc.me, 1, ch, slot, pc.yp).wait_send()

            @pl.when(pc.inner)
            def _():
                for slot in (2, 9, 10):
                    self.rc(pc.me, 1, ch, 0, pc.yp, slot).wait_send()

            @pl.when(pc.end)
            def _():
                self.rc(pc.me, 1, ch, 1, pc.yp).wait_send()
            for slot in (7, 8):
                self.rc(pc.own, 4, ch, slot, pc.sib).wait_send()
        loop(NA, body)

    def run(self, consume, after_a=None, hook=None):
        def body(s):
            @pl.when(s < NA)
            def _():
                self.a(s)

            if after_a is not None:
                @pl.when(s == NA)
                def _():
                    after_a()

            @pl.when((s >= 1) & (s <= NA))
            def _():
                self.b(s - 1)

            if hook is not None:
                hook(s)

            @pl.when(s >= 2)
            def _():
                self.c(s - 2)
                if consume is not None:
                    consume(s - 2)
        loop(NA + 2, body)
        self.finish()


class Scatter:
    def __init__(self, pc, part, bufs, send, recv, out):
        self.pc, self.part, self.send, self.recv, self.out = pc, part, send, recv, out
        self.ra, self.sb, self.rb, self.sc, self.rcv = bufs
        self.cw = part.shape[2] // NR

    def cols(self, ch):
        return pl.ds(pl.multiple_of(ch * self.cw, self.cw), self.cw)

    def copy(self, src, dst, ch, slot, dev):
        return remote(src, dst, self.send.at[ch, slot], self.recv.at[ch, slot], dev)

    def to_sib(self, ch):
        pc = self.pc
        return self.copy(self.part.at[pl.ds((1 - pc.c) * 8, 8), :, self.cols(ch)],
                         self.ra.at[:, :, self.cols(ch)], ch, 0, pc.sib)

    def to_y(self, ch):
        return self.copy(self.sb.at[:, :, self.cols(ch)], self.rb.at[:, :, self.cols(ch)], ch, 1, self.pc.yp)

    def to_z(self, ch, k):
        return self.copy(self.sc.at[k - 1, :, self.cols(ch)], self.rcv.at[k - 1, :, self.cols(ch)],
                         ch, 1 + k, self.pc.tz[k])

    def s0(self, ch):
        self.to_sib(ch).start()

    def s1(self, ch):
        pc, cols = self.pc, self.cols(ch)
        self.to_sib(ch).wait_recv()
        for k in range(4):
            self.sb[k, :, cols] = (self.part[pc.oth + k, :, cols].astype(F32)
                                   + self.ra[(1 - pc.y) * 4 + k, :, cols].astype(F32)).astype(BF16)
        self.to_y(ch).start()

    def pair(self, zk, cols):
        pc = self.pc
        return (self.part[pc.own + zk, :, cols].astype(F32) + self.ra[pc.y * 4 + zk, :, cols].astype(F32)
                + self.rb[zk, :, cols].astype(F32))

    def s2(self, ch):
        pc, cols = self.pc, self.cols(ch)
        self.to_y(ch).wait_recv()
        for k in (2, 3, 1):
            self.sc[k - 1, :, cols] = self.pair(pc.zs[k], cols).astype(BF16)
            self.to_z(ch, k).start()

    def s3(self, ch):
        pc, cols = self.pc, self.cols(ch)
        acc = self.pair(pc.z, cols)
        for k in (1, 2, 3):
            self.to_z(ch, k).wait_recv()
            acc = acc + self.rcv[k - 1, :, cols].astype(F32)
        self.out[:, cols] = acc

    def finish(self):
        def body(ch):
            self.to_sib(ch).wait_send()
            self.to_y(ch).wait_send()
            for k in (1, 2, 3):
                self.to_z(ch, k).wait_send()
        loop(NR, body)

    def run(self, compute, hook=None, mid=None):
        def front(s):
            @pl.when(s < NR)
            def _():
                compute(s)
                self.s0(s)

            @pl.when(s >= 1)
            def _():
                self.s1(s - 1)
        loop(NR + 1, front)

        def back(s):
            if hook is not None:
                hook(s)
            self.s2(s)
        loop(NR, back)
        if mid is not None:
            mid()
        loop(NR, self.s3)
        self.finish()


class SmallSum:
    def __init__(self, pc, rows_f32, vals, ra, sb, rb, rz, total, send, recv):
        self.pc, self.rows, self.vals, self.ra, self.sb, self.rb, self.rz = pc, rows_f32, vals, ra, sb, rb, rz
        self.total, self.send, self.recv = total, send, recv
        self.half = vals.shape[1] // 2

    def cols(self, core):
        return pl.ds(pl.multiple_of(core * self.half, self.half), self.half)

    def copy(self, src, dst, slot, dev):
        return remote(src, dst, self.send.at[slot], self.recv.at[slot], dev)

    def to_sib(self):
        return self.copy(self.vals.at[:, self.cols(1 - self.pc.c)], self.ra, 0, self.pc.sib)

    def to_y(self):
        return self.copy(self.sb, self.rb, 1, self.pc.yp)

    def to_z(self, k):
        return self.copy(self.rz.at[self.pc.z], self.rz.at[self.pc.z], 1 + k, self.pc.tz[k])

    def back(self):
        ref = self.total.at[:, self.cols(self.pc.c)]
        return self.copy(ref, ref, 5, self.pc.sib)

    def t0(self):
        self.vals[ALL] = self.rows[ALL].astype(BF16)
        self.to_sib().start()

    def t1(self):
        self.to_sib().wait_recv()
        self.sb[ALL] = (self.vals[:, self.cols(self.pc.c)].astype(F32) + self.ra[ALL].astype(F32)).astype(BF16)
        self.to_y().start()

    def t2(self):
        self.to_y().wait_recv()
        self.rz[self.pc.z] = (self.sb[ALL].astype(F32) + self.rb[ALL].astype(F32)).astype(BF16)
        for k in (1, 2, 3):
            self.to_z(k).start()

    def t3(self):
        for k in (1, 2, 3):
            self.to_z(k).wait_recv()
        self.total[:, self.cols(self.pc.c)] = jnp.sum(self.rz[ALL].astype(F32), axis=0)
        self.back().start()

    def t4(self):
        self.back().wait_recv()
        self.back().wait_send()
        self.to_sib().wait_send()
        self.to_y().wait_send()
        for k in (1, 2, 3):
            self.to_z(k).wait_send()


def block_of(t):
    return (t % 2) * 8 + (t // 2 % 2) * 4 + t // 4


def chain_kernel(ids, slopes, eg, eb, g1, b1, g2, b2, bd, bf2, bqkv, bf1, dout,
                 table_h, wqkv_h, wd_h, w1_h, w2_h,
                 h1_o, h2_o, dy_o, dr_o, dx_o, ctx_o, gelu_o, dpre_o, dqkv_o, y_o, small_o, dbf1_o, dbqkv_o,
                 table, wraw, wq, wd, w1, w2, h1, h2, dy, dr, dx, part, party,
                 ra, sb, rb, sc, rcv, yra, ysb, yrb, ysc, yrcv,
                 onehot, wstage, qkv_acc, qkv, prob, ctx, pre, dgelu, gelu_bf, dpre, dqkv,
                 rsum, e_val, e_hat, n1_hat, n2_hat, r_one, dr_own, invs,
                 stat, sv, sra, ssb, srb, srz, stot,
                 lsem, osem, ags, agr, agds, agdr, rss, rsr, rsys, rsyr, sts, strc):
    pc = Place()
    dim = table.shape[1]
    vocab_rows = table.shape[0]
    ra_w, rs_w, wq_w = dim // NA, dim // NR, dim // NW

    loads = [pltpu.make_async_copy(table_h, table, lsem.at[0]),
             pltpu.make_async_copy(wd_h, wd, lsem.at[1]),
             pltpu.make_async_copy(w1_h, w1, lsem.at[2]),
             pltpu.make_async_copy(w2_h, w2, lsem.at[3])]
    raw_rows = wraw.shape[1]

    def raw_load(ch, slot):
        return pltpu.make_async_copy(wqkv_h.at[pl.ds(pl.multiple_of(ch * raw_rows, raw_rows), raw_rows), :],
                                     wraw.at[slot], lsem.at[4 + slot])

    loads[0].start()
    raw_load(0, 0).start()
    raw_load(1, 1).start()
    for cp in loads[1:]:
        cp.start()

    barrier = pltpu.get_barrier_semaphore()
    partners = [pc.sib, pc.yp] + pc.tz[1:]
    for dev in partners:
        pl.semaphore_signal(barrier, inc=1, device_id={'tp': dev}, device_id_type=MESH)

    local_ids = ids[ALL] - pc.t * vocab_rows
    hit = (local_ids == lax.broadcasted_iota(jnp.int32, (vocab_rows, SEQ), 0)).astype(F32).T.astype(BF16)
    for t in range(NB):
        onehot[block_of(t) * BLK:(block_of(t) + 1) * BLK, :] = hit[t * BLK:(t + 1) * BLK, :]
    pl.semaphore_wait(barrier, len(partners))
    loads[0].wait()

    def ac(ch):
        return pl.ds(pl.multiple_of(ch * ra_w, ra_w), ra_w)

    def rc(ch):
        return pl.ds(pl.multiple_of(ch * rs_w, rs_w), rs_w)

    def blocks(value):
        return value.reshape(NB, BLK, value.shape[1])

    def rows(value):
        return value.reshape(SEQ, value.shape[2])

    main = (ra, sb, rb, sc, rcv)
    side = (yra, ysb, yrb, ysc, yrcv)
    scatter = Scatter(pc, part, main, rss, rsr, rsum)
    scatter_y = Scatter(pc, party, side, rsys, rsyr, rsum)

    def embed(ch):
        part[:, :, rc(ch)] = blocks(dot_nn(onehot[ALL], table[:, rc(ch)]).astype(BF16))

    def unpack_wqkv(s):
        def piece(q):
            p = s * (NW // NR) + q
            slot = lax.rem(p, 2)
            raw_load(p, slot).wait()

            def body(i):
                wstage[ALL] = wraw[slot, pl.ds(pl.multiple_of(i * QKV, QKV), QKV), :].astype(F32)
                out_row = pl.multiple_of(p * wq_w + i * LANE, LANE)
                for j in range(6):
                    wq[pl.ds(out_row, LANE), j * LANE:(j + 1) * LANE] = wstage[pl.ds(j, LANE, stride=6), :].astype(BF16)
            loop(raw_rows // QKV, body)

            @pl.when(p + 2 < NW)
            def _():
                raw_load(p + 2, slot).start()
        loop(NW // NR, piece)

    dy[pc.me] = dout[ALL]
    gather_dy = Gather(pc, dy, agds, agdr)
    scatter.run(embed, unpack_wqkv, gather_dy.start_y)
    e_norm, hat, inv = norm_forward(rsum[ALL], eg[ALL], eb[ALL])
    e_hat[ALL] = hat
    invs[0] = jnp.broadcast_to(inv, (BLK, LANE))
    embedded = e_norm.astype(BF16).astype(F32)
    e_val[ALL] = embedded
    n1_norm, hat, inv = norm_forward(embedded, g1[ALL], b1[ALL])
    n1_hat[ALL] = hat
    invs[1] = jnp.broadcast_to(inv, (BLK, LANE))
    h1[pc.me] = n1_norm.astype(BF16)

    gather = Gather(pc, h1, ags, agr)
    gather.start()
    qkv_acc[ALL] = jnp.zeros_like(qkv_acc)

    def use_h1(ch):
        qkv_acc[ALL] += dot_nn(rows(h1[:, :, ac(ch)]), wq[ac(ch), :])

    gather.run(use_h1, gather_dy.start_z)
    out_h1 = pltpu.make_async_copy(h1, h1_o, osem.at[0])
    out_h1.start()

    def position(axis):
        r = lax.broadcasted_iota(jnp.int32, (SEQ, SEQ), axis)
        core, yy = lax.shift_right_logical(r, 7), lax.shift_right_logical(r, 6) & 1
        zz, w = lax.shift_right_logical(r, 4) & 3, r & 15
        return zz * 64 + yy * 32 + core * 16 + w

    q_pos, k_pos = position(0), position(1)
    rel = (k_pos - q_pos).astype(F32)
    causal = k_pos <= q_pos
    scale = LANE ** -0.5

    for j in range(6):
        qkv[:, j * LANE:(j + 1) * LANE] = (qkv_acc[:, j * LANE:(j + 1) * LANE] + bqkv[j // 2, j % 2:j % 2 + 1, :]).astype(BF16)

    def head_cols(kind, h):
        return slice((kind * 2 + h) * LANE, (kind * 2 + h + 1) * LANE)

    def attend(h):
        scores = dot_nt(qkv[:, head_cols(0, h)], qkv[:, head_cols(1, h)]) * scale
        scores = jnp.where(causal, scores + slopes[pc.t * 2 + h] * rel, -1e30)
        ex = jnp.exp(scores - jnp.max(scores, axis=-1, keepdims=True))
        p = ex / jnp.sum(ex, axis=-1, keepdims=True)
        prob[h] = p
        ctx[:, h * LANE:(h + 1) * LANE] = dot_nn(p.astype(BF16), qkv[:, head_cols(2, h)]).astype(BF16)

    attend(0)
    attend(1)
    loop(NA // 2, gather_dy.a)
    loads[1].wait()

    def dense(ch):
        part[:, :, rc(ch)] = blocks(dot_nn(ctx[ALL], wd[:, rc(ch)]).astype(BF16))

    def dy_rest():
        loop(NA // 2, lambda ch: gather_dy.a(NA // 2 + ch))
        loop(NA // 2, gather_dy.b)

    scatter.run(dense, None, dy_rest)
    out_ctx = pltpu.make_async_copy(ctx, ctx_o, osem.at[2])
    out_ctx.start()

    r_val = (e_val[ALL] + rsum[ALL] + bd[ALL]).astype(BF16).astype(F32)
    r_one[ALL] = r_val
    n2_norm, hat, inv = norm_forward(r_val, g2[ALL], b2[ALL])
    n2_hat[ALL] = hat
    invs[2] = jnp.broadcast_to(inv, (BLK, LANE))
    h2[pc.me] = n2_norm.astype(BF16)
    gather = Gather(pc, h2, ags, agr)
    gather.start()
    pre[ALL] = jnp.zeros_like(pre)
    dgelu[ALL] = jnp.zeros_like(dgelu)
    loads[2].wait()
    loads[3].wait()

    def use_h2(ch):
        pre[ALL] += dot_nn(rows(h2[:, :, ac(ch)]), w1[ac(ch), :])

    def use_dy(s):
        @pl.when(s < NA)
        def _():
            @pl.when(s < NA // 2)
            def _():
                gather_dy.b(NA // 2 + s)
            gather_dy.c(s)
            dgelu[ALL] += dot_nt(rows(dy[:, :, ac(s)]), w2[:, ac(s)])

    gather.run(use_h2, None, use_dy)
    gather_dy.finish()
    out_dy = pltpu.make_async_copy(dy, dy_o, osem.at[1])
    out_dy.start()
    out_h2 = pltpu.make_async_copy(h2, h2_o, osem.at[3])
    out_h2.start()

    def act(i, total):
        rs = pl.ds(pl.multiple_of(i * 32, 32), 32)
        x = pre[rs, :] + bf1[ALL]
        th = jnp.tanh(GELU_A * (x + GELU_B * (x * x * x)))
        cdf = 0.5 * (1.0 + th)
        gelu_bf[rs, :] = (x * cdf).astype(BF16)
        slope = cdf + x * (0.5 * (1.0 - th * th)) * (GELU_A * (1.0 + 3.0 * GELU_B * (x * x)))
        d = dgelu[rs, :] * slope
        dpre[rs, :] = d.astype(BF16)
        return total + jnp.sum(d, axis=0, keepdims=True)

    dbf1_o[ALL] = lax.fori_loop(0, SEQ // 32, act, jnp.zeros((1, pre.shape[1]), F32))
    out_gelu = pltpu.make_async_copy(gelu_bf, gelu_o, osem.at[4])
    out_gelu.start()
    out_dpre = pltpu.make_async_copy(dpre, dpre_o, osem.at[5])
    out_dpre.start()

    def dh2(ch):
        part[:, :, rc(ch)] = blocks(dot_nt(dpre[ALL], w1[rc(ch), :]).astype(BF16))

    def mlp(s):
        party[:, :, rc(s)] = blocks(dot_nn(gelu_bf[ALL], w2[:, rc(s)]).astype(BF16))
        scatter_y.s0(s)

    scatter.run(dh2, mlp, lambda: loop(NR // 2, scatter_y.s1))
    dn, sg, sbv = norm_backward(rsum[ALL], n2_hat[ALL], invs[2, :, 0:1], g2[ALL])
    dr_val = dout[ALL].astype(F32) + dn
    dr_own[ALL] = dr_val
    dr[pc.me] = dr_val.astype(BF16)
    stat[ALL] = jnp.zeros_like(stat)
    stat[4:5, :] = sg
    stat[5:6, :] = sbv
    gather = Gather(pc, dr, ags, agr)
    gather.start()
    d_ctx = qkv_acc.at[:, 0:256]
    d_ctx[ALL] = jnp.zeros((SEQ, 256), F32)

    def use_dr(ch):
        d_ctx[ALL] += dot_nt(rows(dr[:, :, ac(ch)]), wd[:, ac(ch)])

    gather.run(use_dr, lambda: loop(NR // 2, scatter_y.s2))
    out_dr = pltpu.make_async_copy(dr, dr_o, osem.at[6])
    out_dr.start()
    loop(NR // 4, lambda ch: scatter_y.s1(NR // 2 + ch))

    def attend_back(h):
        dc = d_ctx[:, h * LANE:(h + 1) * LANE].astype(BF16)
        p = prob[h]
        d_value = dot_tn(p.astype(BF16), dc)
        d_prob = dot_nt(dc, qkv[:, head_cols(2, h)])
        ds = p * (d_prob - jnp.sum(d_prob * p, axis=-1, keepdims=True))
        ds_bf = (ds * scale).astype(BF16)
        d_query = dot_nn(ds_bf, qkv[:, head_cols(1, h)])
        d_key = dot_tn(ds_bf, qkv[:, head_cols(0, h)])
        for kind, val in ((0, d_query), (1, d_key), (2, d_value)):
            dqkv[:, head_cols(kind, h)] = val.astype(BF16)
            dbqkv_o[kind, h:h + 1, :] = jnp.sum(val, axis=0, keepdims=True)

    attend_back(0)
    attend_back(1)
    out_dqkv = pltpu.make_async_copy(dqkv, dqkv_o, osem.at[7])
    out_dqkv.start()
    def dh1(ch):
        part[:, :, rc(ch)] = blocks(dot_nt(dqkv[ALL], wq[rc(ch), :]).astype(BF16))

    def y_more():
        loop(NR // 4, lambda ch: scatter_y.s1(NR * 3 // 4 + ch))
        loop(NR // 4, lambda ch: scatter_y.s2(NR // 2 + ch))

    scatter.run(dh1, None, y_more)
    dn, sg1, sb1 = norm_backward(rsum[ALL], n1_hat[ALL], invs[1, :, 0:1], g1[ALL])
    dxv, sg0, sb0 = norm_backward(dr_own[ALL] + dn, e_hat[ALL], invs[0, :, 0:1], eg[ALL])
    dx[pc.me] = dxv.astype(BF16)
    for i, row in enumerate((sg0, sb0, sg1, sb1)):
        stat[i:i + 1, :] = row
    sums = SmallSum(pc, stat, sv, sra, ssb, srb, srz, stot, sts, strc)
    sums.t0()
    gather = Gather(pc, dx, ags, agr)
    gather.start()

    def sums_step(s):
        for i, step in enumerate((sums.t1, sums.t2, sums.t3)):
            pl.when(s == i)(step)

        @pl.when(s < NA)
        def _():
            small_o[6:7, ac(s)] = jnp.sum(rows(dr[:, :, ac(s)]).astype(F32), axis=0, keepdims=True)
            small_o[7:8, ac(s)] = jnp.sum(rows(dy[:, :, ac(s)]).astype(F32), axis=0, keepdims=True)

    gather.run(None, lambda: loop(NR // 4, lambda ch: scatter_y.s2(NR * 3 // 4 + ch)), sums_step)
    outs = [pltpu.make_async_copy(dx.at[block_of(t)], dx_o.at[t], osem.at[8]) for t in range(NB)]
    for cp in outs:
        cp.start()
    loop(NR, scatter_y.s3)
    scatter_y.finish()
    y_o[ALL] = (r_one[ALL] + rsum[ALL] + bf2[ALL]).astype(BF16)
    sums.t4()
    small_o[0:6, :] = stot[0:6, :]
    for cp in (out_h1, out_dy, out_ctx, out_h2, out_gelu, out_dpre, out_dr, out_dqkv):
        cp.wait()
    pltpu.make_async_copy(dx, dx_o, osem.at[8]).wait()


def chain(ids, slopes, vecs, bqkv, bf1, dout, table, wqkv, wd, w1, w2):
    vocab_rows, dim = table.shape
    ff = w1.shape[1]
    act = jax.ShapeDtypeStruct((NB, BLK, dim), BF16)
    out_shape = [act] * 5 + [
        jax.ShapeDtypeStruct((SEQ, 256), BF16), jax.ShapeDtypeStruct((SEQ, ff), BF16),
        jax.ShapeDtypeStruct((SEQ, ff), BF16), jax.ShapeDtypeStruct((SEQ, QKV), BF16),
        jax.ShapeDtypeStruct((BLK, dim), BF16), jax.ShapeDtypeStruct((8, dim), F32),
        jax.ShapeDtypeStruct((1, ff), F32), jax.ShapeDtypeStruct((3, 2, LANE), F32)]
    vmem, hbm = pl.BlockSpec(memory_space=pltpu.VMEM), pl.BlockSpec(memory_space=pl.ANY)
    full = pltpu.VMEM((NB, BLK, dim), BF16)
    rs_bufs = [pltpu.VMEM((8, BLK, dim), BF16), pltpu.VMEM((4, BLK, dim), BF16), pltpu.VMEM((4, BLK, dim), BF16),
               pltpu.VMEM((3, BLK, dim), BF16), pltpu.VMEM((3, BLK, dim), BF16)]
    row = pltpu.VMEM((BLK, dim), F32)
    dma = pltpu.SemaphoreType.DMA
    scratch = [pltpu.VMEM((vocab_rows, dim), BF16), pltpu.VMEM((2, dim * 6 // NW, LANE), BF16),
               pltpu.VMEM((dim, QKV), BF16), pltpu.VMEM(wd.shape, BF16), pltpu.VMEM(w1.shape, BF16),
               pltpu.VMEM(w2.shape, BF16), full, full, full, full, full,
               full, full]
    scratch += rs_bufs + rs_bufs
    scratch += [pltpu.VMEM((SEQ, vocab_rows), BF16), pltpu.VMEM((QKV, LANE), F32), pltpu.VMEM((SEQ, QKV), F32),
                pltpu.VMEM((SEQ, QKV), BF16), pltpu.VMEM((2, SEQ, SEQ), F32), pltpu.VMEM((SEQ, 256), BF16),
                pltpu.VMEM((SEQ, ff), F32), pltpu.VMEM((SEQ, ff), F32), pltpu.VMEM((SEQ, ff), BF16),
                pltpu.VMEM((SEQ, ff), BF16), pltpu.VMEM((SEQ, QKV), BF16)]
    scratch += [row] * 7 + [pltpu.VMEM((3, BLK, LANE), F32)]
    half = pltpu.VMEM((8, dim // 2), BF16)
    scratch += [pltpu.VMEM((8, dim), F32), pltpu.VMEM((8, dim), BF16), half, half, half,
                pltpu.VMEM((4, 8, dim // 2), BF16), pltpu.VMEM((8, dim), F32)]
    scratch += [dma((6,)), dma((9,))] + [dma((NA, 11)), dma((NA, 9))] * 2 + [dma((NR, 5))] * 4 + [dma((6,))] * 2
    return pl.pallas_call(
        chain_kernel, out_shape=out_shape,
        in_specs=[vmem, pl.BlockSpec(memory_space=pltpu.SMEM)] + [vmem] * 11 + [hbm] * 5,
        out_specs=[hbm] * 9 + [vmem] * 4,
        scratch_shapes=scratch, name='chain',
        compiler_params=pltpu.CompilerParams(collective_id=1, has_side_effects=True,
                                             vmem_limit_bytes=67043328),
    )(ids, slopes, *vecs, bqkv, bf1, dout, table, wqkv, wd, w1, w2)


def qkv_grad_kernel(h1, dqkv, out, stage):
    n = h1.shape[1]
    for j in range(6):
        stage[pl.ds(j, n, stride=6), :] = dot_tn(h1[ALL], dqkv[:, j * LANE:(j + 1) * LANE])
    out[ALL] = stage[ALL].astype(BF16)


def qkv_grad(h1, dqkv):
    dim = h1.shape[1]
    step = 512
    return pl.pallas_call(
        qkv_grad_kernel, out_shape=jax.ShapeDtypeStruct((dim * 6, LANE), BF16), grid=(dim // step,),
        in_specs=[pl.BlockSpec((SEQ, step), lambda i: (0, i)), pl.BlockSpec((SEQ, QKV), lambda i: (0, 0))],
        out_specs=pl.BlockSpec((step * 6, LANE), lambda i: (i, 0)),
        scratch_shapes=[pltpu.VMEM((step * 6, LANE), F32)], name='qkv_grad')(h1, dqkv)


def device_step(token_ids, embed_table, emb_gain, emb_bias, ln1_gain, ln1_bias,
                w_qkv, b_qkv, w_dense, b_dense, ln2_gain, ln2_bias,
                w_fc1, b_fc1, w_fc2, b_fc2, d_out, slopes_all):
    dim = embed_table.shape[1]
    vocab_rows = embed_table.shape[0]
    vecs = [v.reshape(1, dim) for v in (emb_gain, emb_bias, ln1_gain, ln1_bias, ln2_gain, ln2_bias, b_dense, b_fc2)]
    wqkv = w_qkv.transpose(0, 2, 1, 3).reshape(dim * 6, LANE)
    (h1, h2, dy, dr, dx, ctx, gelu, dpre, dqkv, y, small, dbf1, dbqkv) = chain(
        token_ids, slopes_all, vecs, b_qkv.transpose(1, 0, 2), b_fc1.reshape(1, -1), d_out.reshape(BLK, dim),
        embed_table, wqkv, w_dense, w_fc1, w_fc2)
    h1, h2, dy, dr, dx = (v.reshape(SEQ, dim) for v in (h1, h2, dy, dr, dx))
    d_w_qkv = qkv_grad(h1, dqkv).reshape(dim, 3, 2, LANE).transpose(0, 2, 1, 3)
    d_w_fc2 = dot_tn(gelu, dy).astype(BF16)
    d_w_fc1 = dot_tn(h2, dpre).astype(BF16)
    d_w_dense = dot_tn(ctx, dr).astype(BF16)
    one_hot = (token_ids - lax.axis_index('tp') * vocab_rows == jnp.arange(vocab_rows)[:, None]).astype(BF16)
    d_table = dot_nn(one_hot, dx)
    return (y[None], d_table, small[0], small[1], small[2], small[3],
            d_w_qkv, dbqkv.transpose(1, 0, 2), d_w_dense, small[6], small[4], small[5],
            d_w_fc1, dbf1.reshape(-1), d_w_fc2, small[7])


def solution(mesh):
    in_specs = (P('dp', None), P('tp', None), P(None), P(None), P(None), P(None),
                P(None, 'tp', None, None), P('tp', None, None), P('tp', None), P(None),
                P(None), P(None), P(None, 'tp'), P('tp'), P('tp', None), P(None),
                P('dp', 'tp', None), P(None))
    out_specs = (P('dp', 'tp', None), P(('dp', 'tp'), None), P('dp'), P('dp'), P('dp'), P('dp'),
                 P('dp', 'tp', None, None), P(('dp', 'tp'), None, None), P(('dp', 'tp'), None), P('dp'),
                 P('dp'), P('dp'), P('dp', 'tp'), P(('dp', 'tp')), P(('dp', 'tp'), None), P('dp'))
    mapped = jax.shard_map(device_step, mesh=mesh, in_specs=in_specs, out_specs=out_specs, check_vma=False)

    def run(*arrays):
        slopes_all = alibi_slopes(arrays[6].shape[1])
        return mapped(*arrays, slopes_all)

    return run
```

```python
import functools
import jax
import jax.numpy as jnp
from jax import lax
from jax.experimental import pallas as pl
from jax.experimental.pallas import tpu as pltpu
from jax.sharding import PartitionSpec as P

EPS = 1e-5
MESH = pl.DeviceIdType.MESH
F32 = jnp.float32
BF16 = jnp.bfloat16
NA = 4
NR = 4
NW = 4
NB = 16
BLK = 16
SEQ = 256
LANE = 128
QKV = 6 * LANE
ALL = slice(None)
GELU_A = 0.7978845608028654
GELU_B = 0.044715


def alibi_slopes(head_count):
    closest = 2 ** (head_count.bit_length() - 1)
    slope_base = 2.0 ** (-8.0 / closest)
    extra_base = 2.0 ** (-4.0 / closest)
    slopes = [slope_base ** exponent for exponent in range(1, closest + 1)]
    slopes = slopes + [extra_base ** exponent for exponent in range(1, 2 * (head_count - closest), 2)]
    return jnp.array(slopes, dtype=jnp.float32)


def norm_forward(values, gain_vec, bias_vec):
    centered = values - jnp.mean(values, axis=-1, keepdims=True)
    inv_std = lax.rsqrt(jnp.mean(centered * centered, axis=-1, keepdims=True) + EPS)
    x_hat = centered * inv_std
    return x_hat * gain_vec + bias_vec, x_hat, inv_std


def norm_backward(d_norm, x_hat, inv_std, gain_vec):
    d_hat = d_norm * gain_vec
    d_values = inv_std * (d_hat - jnp.mean(d_hat, axis=-1, keepdims=True)
                          - x_hat * jnp.mean(d_hat * x_hat, axis=-1, keepdims=True))
    return d_values, jnp.sum(d_norm * x_hat, axis=0, keepdims=True), jnp.sum(d_norm, axis=0, keepdims=True)


def dot_nn(a, b):
    return lax.dot_general(a, b, (((1,), (0,)), ((), ())), preferred_element_type=F32)


def dot_nt(a, b):
    return lax.dot_general(a, b, (((1,), (1,)), ((), ())), preferred_element_type=F32)


def dot_tn(a, b):
    return lax.dot_general(a, b, (((0,), (0,)), ((), ())), preferred_element_type=F32)


class Place:
    def __init__(self):
        t = lax.axis_index('tp')
        self.t = t
        self.c = lax.rem(t, 2)
        self.y = lax.rem(lax.div(t, 2), 2)
        self.z = lax.div(t, 4)
        self.inner = (self.z == 1) | (self.z == 2)
        self.end = (self.z == 0) | (self.z == 3)
        self.sib = t + 1 - 2 * self.c
        self.yp = t + 2 - 4 * self.y
        self.zs = [self.z, self.z + 1 - 2 * lax.rem(self.z, 2), lax.rem(self.z + 2, 4), 3 - self.z]
        self.tz = [zk * 4 + self.y * 2 + self.c for zk in self.zs]
        self.own = self.c * 8 + self.y * 4
        self.oth = self.c * 8 + (1 - self.y) * 4
        self.me = self.own + self.z


def remote(src, dst, send_sem, recv_sem, dev):
    return pltpu.make_async_remote_copy(src_ref=src, dst_ref=dst, send_sem=send_sem, recv_sem=recv_sem,
                                        device_id={'tp': dev}, device_id_type=MESH)


def loop(n, fn):
    def body(i, carry):
        fn(i)
        return carry
    lax.fori_loop(0, n, body, 0)


class Gather:
    def __init__(self, pc, buf, send, recv):
        self.pc, self.buf, self.send, self.recv = pc, buf, send, recv
        self.cw = buf.shape[2] // NA

    def rc(self, first, count, ch, slot, dev, send_slot=None):
        ref = self.buf.at[pl.ds(first, count), :, pl.ds(pl.multiple_of(ch * self.cw, self.cw), self.cw)]
        send_slot = slot if send_slot is None else send_slot
        return remote(ref, ref, self.send.at[ch, send_slot], self.recv.at[ch, slot], dev)

    def block(self, k, ch):
        return self.rc(self.pc.own + self.pc.zs[k], 1, ch, k - 1, self.pc.tz[k])

    def start_y(self):
        loop(NA, lambda ch: self.rc(self.pc.me, 1, ch, 3, self.pc.yp).start())

    def start_z(self):
        pc = self.pc

        def body(ch):
            self.rc(pc.me, 1, ch, 0, pc.tz[1]).start()

            @pl.when(pc.inner)
            def _():
                self.rc(pc.me, 1, ch, 2, pc.tz[3]).start()

            @pl.when(pc.end)
            def _():
                self.rc(pc.me, 1, ch, 1, pc.tz[2]).start()
        loop(NA, body)

    def start(self):
        self.start_y()
        self.start_z()

    def to_y(self, k, ch):
        self.rc(self.pc.own + self.pc.zs[k], 1, ch, 3 + k, self.pc.yp).start()

    def to_end(self, k, ch):
        self.rc(self.pc.own + self.pc.zs[k], 1, ch, 4 - k, self.pc.tz[1], 7 + k).start()

    def a(self, ch):
        pc = self.pc
        self.block(1, ch).wait_recv()
        self.to_y(1, ch)

        @pl.when(pc.inner)
        def _():
            for k in (3, 2):
                self.block(k, ch).wait_recv()
                self.to_end(k, ch)
                self.to_y(k, ch)

        @pl.when(pc.end)
        def _():
            for k in (2, 3):
                self.block(k, ch).wait_recv()
                self.to_y(k, ch)
        self.rc(pc.own, 4, ch, 7, pc.sib).start()

    def b(self, ch):
        pc = self.pc
        for k in range(4):
            self.rc(pc.oth + pc.zs[k], 1, ch, 3 + k, pc.yp).wait_recv()
        self.rc(pc.oth, 4, ch, 8, pc.sib).start()

    def c(self, ch):
        pc = self.pc
        self.rc(pc.own, 4, ch, 7, pc.sib).wait_recv()
        self.rc(pc.oth, 4, ch, 8, pc.sib).wait_recv()

    def finish(self):
        pc = self.pc

        def body(ch):
            for slot in (0, 3, 4, 5, 6):
                self.rc(pc.me, 1, ch, slot, pc.yp).wait_send()

            @pl.when(pc.inner)
            def _():
                for slot in (2, 9, 10):
                    self.rc(pc.me, 1, ch, 0, pc.yp, slot).wait_send()

            @pl.when(pc.end)
            def _():
                self.rc(pc.me, 1, ch, 1, pc.yp).wait_send()
            for slot in (7, 8):
                self.rc(pc.own, 4, ch, slot, pc.sib).wait_send()
        loop(NA, body)

    def run(self, consume, after_a=None, hook=None):
        def body(s):
            @pl.when(s < NA)
            def _():
                self.a(s)

            if after_a is not None:
                @pl.when(s == NA)
                def _():
                    after_a()

            @pl.when((s >= 1) & (s <= NA))
            def _():
                self.b(s - 1)

            if hook is not None:
                hook(s)

            @pl.when(s >= 2)
            def _():
                self.c(s - 2)
                if consume is not None:
                    consume(s - 2)
        loop(NA + 2, body)
        self.finish()


class Scatter:
    def __init__(self, pc, part, bufs, send, recv, out):
        self.pc, self.part, self.send, self.recv, self.out = pc, part, send, recv, out
        self.ra, self.sb, self.rb, self.sc, self.rcv = bufs
        self.cw = part.shape[2] // NR

    def cols(self, ch):
        return pl.ds(pl.multiple_of(ch * self.cw, self.cw), self.cw)

    def copy(self, src, dst, ch, slot, dev):
        return remote(src, dst, self.send.at[ch, slot], self.recv.at[ch, slot], dev)

    def to_sib(self, ch):
        pc = self.pc
        return self.copy(self.part.at[pl.ds((1 - pc.c) * 8, 8), :, self.cols(ch)],
                         self.ra.at[:, :, self.cols(ch)], ch, 0, pc.sib)

    def to_y(self, ch):
        return self.copy(self.sb.at[:, :, self.cols(ch)], self.rb.at[:, :, self.cols(ch)], ch, 1, self.pc.yp)

    def to_z(self, ch, k):
        return self.copy(self.sc.at[k - 1, :, self.cols(ch)], self.rcv.at[k - 1, :, self.cols(ch)],
                         ch, 1 + k, self.pc.tz[k])

    def s0(self, ch):
        self.to_sib(ch).start()

    def s1(self, ch):
        pc, cols = self.pc, self.cols(ch)
        self.to_sib(ch).wait_recv()
        for k in range(4):
            self.sb[k, :, cols] = (self.part[pc.oth + k, :, cols].astype(F32)
                                   + self.ra[(1 - pc.y) * 4 + k, :, cols].astype(F32)).astype(BF16)
        self.to_y(ch).start()

    def pair(self, zk, cols):
        pc = self.pc
        return (self.part[pc.own + zk, :, cols].astype(F32) + self.ra[pc.y * 4 + zk, :, cols].astype(F32)
                + self.rb[zk, :, cols].astype(F32))

    def s2(self, ch):
        pc, cols = self.pc, self.cols(ch)
        self.to_y(ch).wait_recv()
        for k in (2, 3, 1):
            self.sc[k - 1, :, cols] = self.pair(pc.zs[k], cols).astype(BF16)
            self.to_z(ch, k).start()

    def s3(self, ch):
        pc, cols = self.pc, self.cols(ch)
        acc = self.pair(pc.z, cols)
        for k in (1, 2, 3):
            self.to_z(ch, k).wait_recv()
            acc = acc + self.rcv[k - 1, :, cols].astype(F32)
        self.out[:, cols] = acc

    def finish(self):
        def body(ch):
            self.to_sib(ch).wait_send()
            self.to_y(ch).wait_send()
            for k in (1, 2, 3):
                self.to_z(ch, k).wait_send()
        loop(NR, body)

    def run(self, compute, hook=None, mid=None):
        def front(s):
            @pl.when(s < NR)
            def _():
                compute(s)
                self.s0(s)

            @pl.when(s >= 1)
            def _():
                self.s1(s - 1)
        loop(NR + 1, front)

        def back(s):
            if hook is not None:
                hook(s)
            self.s2(s)
        loop(NR, back)
        if mid is not None:
            mid()
        loop(NR, self.s3)
        self.finish()


class SmallSum:
    def __init__(self, pc, rows_f32, vals, ra, sb, rb, rz, total, send, recv):
        self.pc, self.rows, self.vals, self.ra, self.sb, self.rb, self.rz = pc, rows_f32, vals, ra, sb, rb, rz
        self.total, self.send, self.recv = total, send, recv
        self.half = vals.shape[1] // 2

    def cols(self, core):
        return pl.ds(pl.multiple_of(core * self.half, self.half), self.half)

    def copy(self, src, dst, slot, dev):
        return remote(src, dst, self.send.at[slot], self.recv.at[slot], dev)

    def to_sib(self):
        return self.copy(self.vals.at[:, self.cols(1 - self.pc.c)], self.ra, 0, self.pc.sib)

    def to_y(self):
        return self.copy(self.sb, self.rb, 1, self.pc.yp)

    def to_z(self, k):
        return self.copy(self.rz.at[self.pc.z], self.rz.at[self.pc.z], 1 + k, self.pc.tz[k])

    def back(self):
        ref = self.total.at[:, self.cols(self.pc.c)]
        return self.copy(ref, ref, 5, self.pc.sib)

    def t0(self):
        self.vals[ALL] = self.rows[ALL].astype(BF16)
        self.to_sib().start()

    def t1(self):
        self.to_sib().wait_recv()
        self.sb[ALL] = (self.vals[:, self.cols(self.pc.c)].astype(F32) + self.ra[ALL].astype(F32)).astype(BF16)
        self.to_y().start()

    def t2(self):
        self.to_y().wait_recv()
        self.rz[self.pc.z] = (self.sb[ALL].astype(F32) + self.rb[ALL].astype(F32)).astype(BF16)
        for k in (1, 2, 3):
            self.to_z(k).start()

    def t3(self):
        for k in (1, 2, 3):
            self.to_z(k).wait_recv()
        self.total[:, self.cols(self.pc.c)] = jnp.sum(self.rz[ALL].astype(F32), axis=0)
        self.back().start()

    def t4(self):
        self.back().wait_recv()
        self.back().wait_send()
        self.to_sib().wait_send()
        self.to_y().wait_send()
        for k in (1, 2, 3):
            self.to_z(k).wait_send()


def block_of(t):
    return (t % 2) * 8 + (t // 2 % 2) * 4 + t // 4


def chain_kernel(ids, slopes, eg, eb, g1, b1, g2, b2, bd, bf2, bqkv, bf1, dout,
                 table_h, wqkv_h, wd_h, w1_h, w2_h,
                 h1_o, h2_o, dy_o, dr_o, dx_o, ctx_o, gelu_o, dpre_o, dqkv_o, y_o, small_o, dbf1_o, dbqkv_o,
                 table, wraw, wq, wd, w1, w2, h1, h2, dy, dr, dx, part, party,
                 ra, sb, rb, sc, rcv, yra, ysb, yrb, ysc, yrcv,
                 onehot, wstage, qkv_acc, qkv, prob, ctx, pre, dgelu, gelu_bf, dpre, dqkv,
                 rsum, e_val, e_hat, n1_hat, n2_hat, r_one, dr_own, invs,
                 stat, sv, sra, ssb, srb, srz, stot,
                 lsem, osem, ags, agr, agds, agdr, rss, rsr, rsys, rsyr, sts, strc):
    pc = Place()
    dim = table.shape[1]
    vocab_rows = table.shape[0]
    ra_w, rs_w, wq_w = dim // NA, dim // NR, dim // NW

    loads = [pltpu.make_async_copy(table_h, table, lsem.at[0]),
             pltpu.make_async_copy(wd_h, wd, lsem.at[1]),
             pltpu.make_async_copy(w1_h, w1, lsem.at[2]),
             pltpu.make_async_copy(w2_h, w2, lsem.at[3])]
    raw_rows = wraw.shape[1]

    def raw_load(ch, slot):
        return pltpu.make_async_copy(wqkv_h.at[pl.ds(pl.multiple_of(ch * raw_rows, raw_rows), raw_rows), :],
                                     wraw.at[slot], lsem.at[4 + slot])

    loads[0].start()
    raw_load(0, 0).start()
    raw_load(1, 1).start()
    for cp in loads[1:]:
        cp.start()

    barrier = pltpu.get_barrier_semaphore()
    partners = [pc.sib, pc.yp] + pc.tz[1:]
    for dev in partners:
        pl.semaphore_signal(barrier, inc=1, device_id={'tp': dev}, device_id_type=MESH)

    local_ids = ids[ALL] - pc.t * vocab_rows
    hit = (local_ids == lax.broadcasted_iota(jnp.int32, (vocab_rows, SEQ), 0)).astype(F32).T.astype(BF16)
    for t in range(NB):
        onehot[block_of(t) * BLK:(block_of(t) + 1) * BLK, :] = hit[t * BLK:(t + 1) * BLK, :]
    pl.semaphore_wait(barrier, len(partners))
    loads[0].wait()

    def ac(ch):
        return pl.ds(pl.multiple_of(ch * ra_w, ra_w), ra_w)

    def rc(ch):
        return pl.ds(pl.multiple_of(ch * rs_w, rs_w), rs_w)

    def blocks(value):
        return value.reshape(NB, BLK, value.shape[1])

    def rows(value):
        return value.reshape(SEQ, value.shape[2])

    main = (ra, sb, rb, sc, rcv)
    side = (yra, ysb, yrb, ysc, yrcv)
    scatter = Scatter(pc, part, main, rss, rsr, rsum)
    scatter_y = Scatter(pc, party, side, rsys, rsyr, rsum)

    def embed(ch):
        part[:, :, rc(ch)] = blocks(dot_nn(onehot[ALL], table[:, rc(ch)]).astype(BF16))

    def unpack_wqkv(s):
        def piece(q):
            p = s * (NW // NR) + q
            slot = lax.rem(p, 2)
            raw_load(p, slot).wait()

            def body(i):
                wstage[ALL] = wraw[slot, pl.ds(pl.multiple_of(i * QKV, QKV), QKV), :].astype(F32)
                out_row = pl.multiple_of(p * wq_w + i * LANE, LANE)
                for j in range(6):
                    wq[pl.ds(out_row, LANE), j * LANE:(j + 1) * LANE] = wstage[pl.ds(j, LANE, stride=6), :].astype(BF16)
            loop(raw_rows // QKV, body)

            @pl.when(p + 2 < NW)
            def _():
                raw_load(p + 2, slot).start()
        loop(NW // NR, piece)

    dy[pc.me] = dout[ALL]
    gather_dy = Gather(pc, dy, agds, agdr)
    scatter.run(embed, unpack_wqkv, gather_dy.start_y)
    e_norm, hat, inv = norm_forward(rsum[ALL], eg[ALL], eb[ALL])
    e_hat[ALL] = hat
    invs[0] = jnp.broadcast_to(inv, (BLK, LANE))
    embedded = e_norm.astype(BF16).astype(F32)
    e_val[ALL] = embedded
    n1_norm, hat, inv = norm_forward(embedded, g1[ALL], b1[ALL])
    n1_hat[ALL] = hat
    invs[1] = jnp.broadcast_to(inv, (BLK, LANE))
    h1[pc.me] = n1_norm.astype(BF16)

    gather = Gather(pc, h1, ags, agr)
    gather.start()
    qkv_acc[ALL] = jnp.zeros_like(qkv_acc)

    def use_h1(ch):
        qkv_acc[ALL] += dot_nn(rows(h1[:, :, ac(ch)]), wq[ac(ch), :])

    gather.run(use_h1, gather_dy.start_z)
    out_h1 = pltpu.make_async_copy(h1, h1_o, osem.at[0])
    out_h1.start()

    def position(axis):
        r = lax.broadcasted_iota(jnp.int32, (SEQ, SEQ), axis)
        core, yy = lax.shift_right_logical(r, 7), lax.shift_right_logical(r, 6) & 1
        zz, w = lax.shift_right_logical(r, 4) & 3, r & 15
        return zz * 64 + yy * 32 + core * 16 + w

    q_pos, k_pos = position(0), position(1)
    rel = (k_pos - q_pos).astype(F32)
    causal = k_pos <= q_pos
    scale = LANE ** -0.5

    for j in range(6):
        qkv[:, j * LANE:(j + 1) * LANE] = (qkv_acc[:, j * LANE:(j + 1) * LANE] + bqkv[j // 2, j % 2:j % 2 + 1, :]).astype(BF16)

    def head_cols(kind, h):
        return slice((kind * 2 + h) * LANE, (kind * 2 + h + 1) * LANE)

    def attend(h):
        scores = dot_nt(qkv[:, head_cols(0, h)], qkv[:, head_cols(1, h)]) * scale
        scores = jnp.where(causal, scores + slopes[pc.t * 2 + h] * rel, -1e30)
        ex = jnp.exp(scores - jnp.max(scores, axis=-1, keepdims=True))
        p = ex / jnp.sum(ex, axis=-1, keepdims=True)
        prob[h] = p
        ctx[:, h * LANE:(h + 1) * LANE] = dot_nn(p.astype(BF16), qkv[:, head_cols(2, h)]).astype(BF16)

    attend(0)
    attend(1)
    loop(NA // 2, gather_dy.a)
    loads[1].wait()

    def dense(ch):
        part[:, :, rc(ch)] = blocks(dot_nn(ctx[ALL], wd[:, rc(ch)]).astype(BF16))

    def dy_rest():
        loop(NA // 2, lambda ch: gather_dy.a(NA // 2 + ch))
        loop(NA // 2, gather_dy.b)

    scatter.run(dense, None, dy_rest)
    out_ctx = pltpu.make_async_copy(ctx, ctx_o, osem.at[2])
    out_ctx.start()

    r_val = (e_val[ALL] + rsum[ALL] + bd[ALL]).astype(BF16).astype(F32)
    r_one[ALL] = r_val
    n2_norm, hat, inv = norm_forward(r_val, g2[ALL], b2[ALL])
    n2_hat[ALL] = hat
    invs[2] = jnp.broadcast_to(inv, (BLK, LANE))
    h2[pc.me] = n2_norm.astype(BF16)
    gather = Gather(pc, h2, ags, agr)
    gather.start()
    pre[ALL] = jnp.zeros_like(pre)
    dgelu[ALL] = jnp.zeros_like(dgelu)
    loads[2].wait()
    loads[3].wait()

    def use_h2(ch):
        pre[ALL] += dot_nn(rows(h2[:, :, ac(ch)]), w1[ac(ch), :])

    def use_dy(s):
        @pl.when(s < NA)
        def _():
            @pl.when(s < NA // 2)
            def _():
                gather_dy.b(NA // 2 + s)
            gather_dy.c(s)
            dgelu[ALL] += dot_nt(rows(dy[:, :, ac(s)]), w2[:, ac(s)])

    gather.run(use_h2, None, use_dy)
    gather_dy.finish()
    out_dy = pltpu.make_async_copy(dy, dy_o, osem.at[1])
    out_dy.start()
    out_h2 = pltpu.make_async_copy(h2, h2_o, osem.at[3])
    out_h2.start()

    def act(i, total):
        rs = pl.ds(pl.multiple_of(i * 32, 32), 32)
        x = pre[rs, :] + bf1[ALL]
        th = jnp.tanh(GELU_A * (x + GELU_B * (x * x * x)))
        cdf = 0.5 * (1.0 + th)
        gelu_bf[rs, :] = (x * cdf).astype(BF16)
        slope = cdf + x * (0.5 * (1.0 - th * th)) * (GELU_A * (1.0 + 3.0 * GELU_B * (x * x)))
        d = dgelu[rs, :] * slope
        dpre[rs, :] = d.astype(BF16)
        return total + jnp.sum(d, axis=0, keepdims=True)

    dbf1_o[ALL] = lax.fori_loop(0, SEQ // 32, act, jnp.zeros((1, pre.shape[1]), F32))
    out_gelu = pltpu.make_async_copy(gelu_bf, gelu_o, osem.at[4])
    out_gelu.start()
    out_dpre = pltpu.make_async_copy(dpre, dpre_o, osem.at[5])
    out_dpre.start()

    def dh2(ch):
        part[:, :, rc(ch)] = blocks(dot_nt(dpre[ALL], w1[rc(ch), :]).astype(BF16))

    def mlp(s):
        party[:, :, rc(s)] = blocks(dot_nn(gelu_bf[ALL], w2[:, rc(s)]).astype(BF16))
        scatter_y.s0(s)

    scatter.run(dh2, mlp, lambda: loop(NR // 2, scatter_y.s1))
    dn, sg, sbv = norm_backward(rsum[ALL], n2_hat[ALL], invs[2, :, 0:1], g2[ALL])
    dr_val = dout[ALL].astype(F32) + dn
    dr_own[ALL] = dr_val
    dr[pc.me] = dr_val.astype(BF16)
    stat[ALL] = jnp.zeros_like(stat)
    stat[4:5, :] = sg
    stat[5:6, :] = sbv
    gather = Gather(pc, dr, ags, agr)
    gather.start()
    d_ctx = qkv_acc.at[:, 0:256]
    d_ctx[ALL] = jnp.zeros((SEQ, 256), F32)

    def use_dr(ch):
        d_ctx[ALL] += dot_nt(rows(dr[:, :, ac(ch)]), wd[:, ac(ch)])

    gather.run(use_dr, lambda: loop(NR // 2, scatter_y.s2))
    out_dr = pltpu.make_async_copy(dr, dr_o, osem.at[6])
    out_dr.start()
    loop(NR // 4, lambda ch: scatter_y.s1(NR // 2 + ch))

    def attend_back(h):
        dc = d_ctx[:, h * LANE:(h + 1) * LANE].astype(BF16)
        p = prob[h]
        d_value = dot_tn(p.astype(BF16), dc)
        d_prob = dot_nt(dc, qkv[:, head_cols(2, h)])
        ds = p * (d_prob - jnp.sum(d_prob * p, axis=-1, keepdims=True))
        ds_bf = (ds * scale).astype(BF16)
        d_query = dot_nn(ds_bf, qkv[:, head_cols(1, h)])
        d_key = dot_tn(ds_bf, qkv[:, head_cols(0, h)])
        for kind, val in ((0, d_query), (1, d_key), (2, d_value)):
            dqkv[:, head_cols(kind, h)] = val.astype(BF16)
            dbqkv_o[kind, h:h + 1, :] = jnp.sum(val, axis=0, keepdims=True)

    attend_back(0)
    attend_back(1)
    out_dqkv = pltpu.make_async_copy(dqkv, dqkv_o, osem.at[7])
    out_dqkv.start()
    def dh1(ch):
        part[:, :, rc(ch)] = blocks(dot_nt(dqkv[ALL], wq[rc(ch), :]).astype(BF16))

    def y_more():
        loop(NR // 4, lambda ch: scatter_y.s1(NR * 3 // 4 + ch))
        loop(NR // 4, lambda ch: scatter_y.s2(NR // 2 + ch))

    scatter.run(dh1, None, y_more)
    dn, sg1, sb1 = norm_backward(rsum[ALL], n1_hat[ALL], invs[1, :, 0:1], g1[ALL])
    dxv, sg0, sb0 = norm_backward(dr_own[ALL] + dn, e_hat[ALL], invs[0, :, 0:1], eg[ALL])
    dx[pc.me] = dxv.astype(BF16)
    for i, row in enumerate((sg0, sb0, sg1, sb1)):
        stat[i:i + 1, :] = row
    sums = SmallSum(pc, stat, sv, sra, ssb, srb, srz, stot, sts, strc)
    sums.t0()
    gather = Gather(pc, dx, ags, agr)
    gather.start()

    def sums_step(s):
        for i, step in enumerate((sums.t1, sums.t2, sums.t3)):
            pl.when(s == i)(step)

        @pl.when(s < NA)
        def _():
            small_o[6:7, ac(s)] = jnp.sum(rows(dr[:, :, ac(s)]).astype(F32), axis=0, keepdims=True)
            small_o[7:8, ac(s)] = jnp.sum(rows(dy[:, :, ac(s)]).astype(F32), axis=0, keepdims=True)

    gather.run(None, lambda: loop(NR // 4, lambda ch: scatter_y.s2(NR * 3 // 4 + ch)), sums_step)
    outs = [pltpu.make_async_copy(dx.at[block_of(t)], dx_o.at[t], osem.at[8]) for t in range(NB)]
    for cp in outs:
        cp.start()
    loop(NR, scatter_y.s3)
    scatter_y.finish()
    y_o[ALL] = (r_one[ALL] + rsum[ALL] + bf2[ALL]).astype(BF16)
    sums.t4()
    small_o[0:6, :] = stot[0:6, :]
    for cp in (out_h1, out_dy, out_ctx, out_h2, out_gelu, out_dpre, out_dr, out_dqkv):
        cp.wait()
    pltpu.make_async_copy(dx, dx_o, osem.at[8]).wait()


def chain(ids, slopes, vecs, bqkv, bf1, dout, table, wqkv, wd, w1, w2):
    vocab_rows, dim = table.shape
    ff = w1.shape[1]
    act = jax.ShapeDtypeStruct((NB, BLK, dim), BF16)
    out_shape = [act] * 5 + [
        jax.ShapeDtypeStruct((SEQ, 256), BF16), jax.ShapeDtypeStruct((SEQ, ff), BF16),
        jax.ShapeDtypeStruct((SEQ, ff), BF16), jax.ShapeDtypeStruct((SEQ, QKV), BF16),
        jax.ShapeDtypeStruct((BLK, dim), BF16), jax.ShapeDtypeStruct((8, dim), F32),
        jax.ShapeDtypeStruct((1, ff), F32), jax.ShapeDtypeStruct((3, 2, LANE), F32)]
    vmem, hbm = pl.BlockSpec(memory_space=pltpu.VMEM), pl.BlockSpec(memory_space=pl.ANY)
    full = pltpu.VMEM((NB, BLK, dim), BF16)
    rs_bufs = [pltpu.VMEM((8, BLK, dim), BF16), pltpu.VMEM((4, BLK, dim), BF16), pltpu.VMEM((4, BLK, dim), BF16),
               pltpu.VMEM((3, BLK, dim), BF16), pltpu.VMEM((3, BLK, dim), BF16)]
    row = pltpu.VMEM((BLK, dim), F32)
    dma = pltpu.SemaphoreType.DMA
    scratch = [pltpu.VMEM((vocab_rows, dim), BF16), pltpu.VMEM((2, dim * 6 // NW, LANE), BF16),
               pltpu.VMEM((dim, QKV), BF16), pltpu.VMEM(wd.shape, BF16), pltpu.VMEM(w1.shape, BF16),
               pltpu.VMEM(w2.shape, BF16), full, full, full, full, full,
               full, full]
    scratch += rs_bufs + rs_bufs
    scratch += [pltpu.VMEM((SEQ, vocab_rows), BF16), pltpu.VMEM((QKV, LANE), F32), pltpu.VMEM((SEQ, QKV), F32),
                pltpu.VMEM((SEQ, QKV), BF16), pltpu.VMEM((2, SEQ, SEQ), F32), pltpu.VMEM((SEQ, 256), BF16),
                pltpu.VMEM((SEQ, ff), F32), pltpu.VMEM((SEQ, ff), F32), pltpu.VMEM((SEQ, ff), BF16),
                pltpu.VMEM((SEQ, ff), BF16), pltpu.VMEM((SEQ, QKV), BF16)]
    scratch += [row] * 7 + [pltpu.VMEM((3, BLK, LANE), F32)]
    half = pltpu.VMEM((8, dim // 2), BF16)
    scratch += [pltpu.VMEM((8, dim), F32), pltpu.VMEM((8, dim), BF16), half, half, half,
                pltpu.VMEM((4, 8, dim // 2), BF16), pltpu.VMEM((8, dim), F32)]
    scratch += [dma((6,)), dma((9,))] + [dma((NA, 11)), dma((NA, 9))] * 2 + [dma((NR, 5))] * 4 + [dma((6,))] * 2
    return pl.pallas_call(
        chain_kernel, out_shape=out_shape,
        in_specs=[vmem, pl.BlockSpec(memory_space=pltpu.SMEM)] + [vmem] * 11 + [hbm] * 5,
        out_specs=[hbm] * 9 + [vmem] * 4,
        scratch_shapes=scratch, name='chain',
        compiler_params=pltpu.CompilerParams(collective_id=1, has_side_effects=True,
                                             vmem_limit_bytes=67043328),
    )(ids, slopes, *vecs, bqkv, bf1, dout, table, wqkv, wd, w1, w2)


def grads_kernel(ids, gelu_h, dy_h, h2_h, dpre_h, h1_h, dqkv_h, ctx_h, dr_h, dx_h, y_h, small_h, dbf1_h, dbqkv_h,
                 y_o, table_o, eg_o, eb_o, g1_o, b1_o, wqkv_o, bqkv_o, wd_o, bd_o, g2_o, b2_o, w1_o, bf1_o, w2_o, bf2_o,
                 gelu, dy, h2, dpre, h1, dqkv, ctx, dr, dx, y, small, dbf1, dbqkv,
                 w2, w1, wqkv, wd, table, stage, isem, osem):
    pairs = ((gelu_h, gelu), (dy_h, dy), (h2_h, h2), (dpre_h, dpre), (h1_h, h1), (dqkv_h, dqkv), (ctx_h, ctx),
             (dr_h, dr), (dx_h, dx), (y_h, y), (small_h, small), (dbf1_h, dbf1), (dbqkv_h, dbqkv))
    loads = [pltpu.make_async_copy(src, dst, isem.at[i]) for i, (src, dst) in enumerate(pairs)]
    for cp in loads:
        cp.start()
    pending = []

    def tiles(count, src, dst, fn):
        slot = len(pending)
        n = src.shape[0] // count

        def body(i):
            tile = pl.ds(pl.multiple_of(i * n, n), n)
            fn(i, tile)
            pltpu.make_async_copy(src.at[tile], dst.at[tile], osem.at[slot]).start()
        loop(count, body)
        pending.append(pltpu.make_async_copy(src, dst, osem.at[slot]))

    def ready(*which):
        for i in which:
            loads[i].wait()

    def lane_tile(i, n):
        return pl.ds(pl.multiple_of(i * n, n), n)

    ready(0, 1)

    def fc2(i, tile):
        w2[tile, :] = dot_tn(gelu[:, tile], dy[ALL]).astype(BF16)
    tiles(4, w2, w2_o, fc2)
    ready(2, 3)

    def fc1(i, tile):
        w1[tile, :] = dot_tn(h2[:, tile], dpre[ALL]).astype(BF16)
    tiles(8, w1, w1_o, fc1)
    ready(8)
    rows_here = table.shape[0]
    local_ids = ids[ALL] - lax.axis_index('tp') * rows_here

    def tab(i, tile):
        n = rows_here // 4
        hit = (local_ids == lax.broadcasted_iota(jnp.int32, (n, SEQ), 0) + i * n).astype(F32).astype(BF16)
        table[tile, :] = dot_nn(hit, dx[ALL])
    tiles(4, table, table_o, tab)
    ready(4, 5)

    def qkv(i, tile):
        n = h1.shape[1] // 8
        for j in range(6):
            stage[pl.ds(j, n, stride=6), :] = dot_tn(h1[:, lane_tile(i, n)], dqkv[:, j * LANE:(j + 1) * LANE])
        wqkv[tile, :] = stage[ALL].astype(BF16)
    tiles(8, wqkv, wqkv_o, qkv)
    ready(6, 7)

    def dense(i, tile):
        wd[tile, :] = dot_tn(ctx[:, tile], dr[ALL]).astype(BF16)
    tiles(2, wd, wd_o, dense)
    ready(9, 10, 11, 12)
    rest = [(y, y_o), (dbf1, bf1_o), (dbqkv, bqkv_o)]
    for i, out in enumerate((eg_o, eb_o, g1_o, b1_o, g2_o, b2_o, bd_o, bf2_o)):
        rest.append((small.at[i:i + 1, :], out))
    for src, dst in rest:
        cp = pltpu.make_async_copy(src, dst, osem.at[len(pending)])
        cp.start()
        pending.append(cp)
    for cp in pending:
        cp.wait()


def grads(ids, gelu, dy, h2, dpre, h1, dqkv, ctx, dr, dx, y, small, dbf1, dbqkv, vocab_rows):
    dim, ff = dy.shape[1], gelu.shape[1]
    ins = (gelu, dy, h2, dpre, h1, dqkv, ctx, dr, dx, y, small, dbf1, dbqkv)

    def sds(*shape, dtype=F32):
        return jax.ShapeDtypeStruct(shape, dtype)
    row = sds(1, dim)
    w2, w1, wqkv, wd = (sds(*shape, dtype=BF16) for shape in ((ff, dim), (dim, ff), (dim * 6, LANE), ctx.shape[1:] + (dim,)))
    table = sds(vocab_rows, dim)
    hbm = pl.BlockSpec(memory_space=pl.ANY)
    out_shape = [sds(*y.shape, dtype=BF16), table, row, row, row, row, wqkv, sds(*dbqkv.shape), wd, row, row, row,
                 w1, sds(1, ff), w2, row]
    scratch = [pltpu.VMEM(v.shape, v.dtype) for v in ins + (w2, w1, wqkv, wd, table)]
    scratch += [pltpu.VMEM((dim * 6 // 8, LANE), F32), pltpu.SemaphoreType.DMA((16,)), pltpu.SemaphoreType.DMA((16,))]
    return pl.pallas_call(
        grads_kernel, out_shape=out_shape,
        in_specs=[pl.BlockSpec(memory_space=pltpu.VMEM)] + [hbm] * len(ins), out_specs=[hbm] * 16,
        scratch_shapes=scratch, name='grads',
        compiler_params=pltpu.CompilerParams(vmem_limit_bytes=67043328))(ids, *ins)


def device_step(token_ids, embed_table, emb_gain, emb_bias, ln1_gain, ln1_bias,
                w_qkv, b_qkv, w_dense, b_dense, ln2_gain, ln2_bias,
                w_fc1, b_fc1, w_fc2, b_fc2, d_out, slopes_all):
    dim = embed_table.shape[1]
    vocab_rows = embed_table.shape[0]
    vecs = [v.reshape(1, dim) for v in (emb_gain, emb_bias, ln1_gain, ln1_bias, ln2_gain, ln2_bias, b_dense, b_fc2)]
    wqkv = w_qkv.transpose(0, 2, 1, 3).reshape(dim * 6, LANE)
    (h1, h2, dy, dr, dx, ctx, gelu, dpre, dqkv, y, small, dbf1, dbqkv) = chain(
        token_ids, slopes_all, vecs, b_qkv.transpose(1, 0, 2), b_fc1.reshape(1, -1), d_out.reshape(BLK, dim),
        embed_table, wqkv, w_dense, w_fc1, w_fc2)
    h1, h2, dy, dr, dx = (v.reshape(SEQ, dim) for v in (h1, h2, dy, dr, dx))
    (y, d_table, d_eg, d_eb, d_g1, d_b1, d_w_qkv, d_b_qkv, d_wd, d_bd, d_g2, d_b2, d_w1, d_bf1, d_w2, d_bf2) = grads(
        token_ids, gelu, dy, h2, dpre, h1, dqkv, ctx, dr, dx, y, small, dbf1, dbqkv, vocab_rows)
    flat = [v.reshape(-1) for v in (d_eg, d_eb, d_g1, d_b1, d_bd, d_g2, d_b2, d_bf1, d_bf2)]
    d_eg, d_eb, d_g1, d_b1, d_bd, d_g2, d_b2, d_bf1, d_bf2 = flat
    return (y[None], d_table, d_eg, d_eb, d_g1, d_b1,
            d_w_qkv.reshape(dim, 3, 2, LANE).transpose(0, 2, 1, 3), d_b_qkv.transpose(1, 0, 2), d_wd, d_bd, d_g2, d_b2,
            d_w1, d_bf1, d_w2, d_bf2)


def solution(mesh):
    in_specs = (P('dp', None), P('tp', None), P(None), P(None), P(None), P(None),
                P(None, 'tp', None, None), P('tp', None, None), P('tp', None), P(None),
                P(None), P(None), P(None, 'tp'), P('tp'), P('tp', None), P(None),
                P('dp', 'tp', None), P(None))
    out_specs = (P('dp', 'tp', None), P(('dp', 'tp'), None), P('dp'), P('dp'), P('dp'), P('dp'),
                 P('dp', 'tp', None, None), P(('dp', 'tp'), None, None), P(('dp', 'tp'), None), P('dp'),
                 P('dp'), P('dp'), P('dp', 'tp'), P(('dp', 'tp')), P(('dp', 'tp'), None), P('dp'))
    mapped = jax.shard_map(device_step, mesh=mesh, in_specs=in_specs, out_specs=out_specs, check_vma=False)

    def run(*arrays):
        slopes_all = alibi_slopes(arrays[6].shape[1])
        return mapped(*arrays, slopes_all)

    return run
```
